32 devices in a mesh: band: 8 (over z, x), img: 4 (over y, core).
Axes of the slice: x: 2, y: 2, z: 4, core: 2. Of those that a mesh axis runs over, the one named last changes fastest.
Arguments:
- pixels: bfloat16 [256, 256, 180], P(('img', 'band')), parts along dimension 0, may hold values from -12 to 12
- keep_mask: int32 [32, 32], P(('img', 'band')), parts along dimension 0, may hold values from 0 to 1, as said below
- band_counts: int32 [32], P(('img', 'band')), parts along dimension 0, may hold values from 0 to 32, as said below
- plan_dest: int32 [32, 16], P(('img', 'band')), parts along dimension 0, may hold values from 0 to 7, as said below
- plan_slot: int32 [32, 16], P(('img', 'band')), parts along dimension 0, may hold values from 0 to 8, as said below
- bias_table: float32 [225, 6], replicated, may hold values from -4 to 4
- gain_attn: float32 [180], replicated, may hold values from 0.25 to 1.75
- qkv_weight: bfloat16 [180, 540], replicated, may hold values from -5 to 5
- proj_weight: bfloat16 [180, 180], replicated, may hold values from -0.4375 to 0.4375
- gain_mlp: float32 [180], replicated, may hold values from 0.25 to 1.75
- hidden_weight: bfloat16 [180, 360], replicated, may hold values from -0.4375 to 0.4375
- output_weight: bfloat16 [360, 180], replicated, may hold values from -0.3125 to 0.3125
Outputs:
- restored: bfloat16 [256, 256, 180], P(('img', 'band')), parts along dimension 0
- work_tiles: bfloat16 [256, 128, 180], P(('img', 'band')), parts along dimension 0
The draws below stay inside these ranges and needn't reach their ends.
There are 4 independent parts, one for each index of `img`. The reference program is written for one: setup_inputs(seed, part) draws one part's arguments, and reference() takes and returns one part's arrays. A program takes and returns all parts, laid end to end along the dimension named above; an argument that names none is the same for every part. Nothing has to cross between parts.
Inputs may be any that keep to these rules, and one draw needn't show every extreme that they name: `keep_mask`: the number of ones in a band varies strongly from band to band. band_counts[b] equals the number of ones among band b's windows in keep_mask. A band's live tiles are those with 2 t < band_counts[b]; their number summed over bands lies between 57 and 64, and some band has all 16 tiles live. `plan_dest`: within each aligned group of 8 consecutive tiles of a band (equal t // 8) the destinations are all different. `plan_slot`: 8 for tiles that are not live; a live tile has a slot below 8, no two live tiles of the image share destination and slot, and some destination receives 8 live tiles.
All inputs are finite; a program needn't handle non-finite values.
Results may differ from the reference program's by a relative error of at most 0.0044.
Values may be sent and summed in bfloat16 or wider, within the bound.
A program may use at most 64 MiB of HBM per device.

```python
import math
import jax
import jax.numpy as jnp
from jax import lax

CHAN = 180
HEADS = 6
FF_WIDTH = 360
WIN = 8
TILE = 2
ROWS = 8
WIDTH = 256
SHIFT = 4
TABLE = 225
HEIGHT = 64
WIN_DEV = 32
TILES_DEV = 16
CAP = 8
N_BAND = 8


def shuffle_band(band_key):
    return jax.random.permutation(band_key, WIN_DEV)


def plan_tables(key):
    key_perm = jax.random.fold_in(key, 101)
    key_share = jax.random.fold_in(key, 102)
    key_cut = jax.random.fold_in(key, 103)
    key_rest = jax.random.fold_in(key, 104)
    key_rank = jax.random.fold_in(key, 105)
    key_turn = jax.random.fold_in(key, 106)
    half_bands = N_BAND // 2
    band_order = jax.random.permutation(key_perm, N_BAND)
    shares = jax.random.randint(key_share, (half_bands,), 1, TILES_DEV + 1).astype(jnp.int32)
    shares = shares.at[0].set(TILES_DEV)
    trimmed = jax.random.randint(key_cut, (), 0, half_bands)
    pair_ids = jnp.arange(half_bands, dtype=jnp.int32)
    lowered = shares - ((pair_ids >= 1) & (pair_ids <= trimmed)).astype(jnp.int32)
    live_tiles = jnp.zeros((N_BAND,), jnp.int32).at[band_order[0::2]].set(lowered).at[band_order[1::2]].set(TILES_DEV - shares)
    spare_windows = jax.random.randint(key_rest, (N_BAND,), 0, TILE).astype(jnp.int32)
    kept_windows = jnp.where(live_tiles > 0, live_tiles * TILE - spare_windows, 0).astype(jnp.int32)
    window_ranks = jax.vmap(shuffle_band)(jax.random.split(key_rank, N_BAND))
    keep_table = (window_ranks < kept_windows[:, None]).astype(jnp.int32).reshape(HEIGHT // WIN, WIDTH // WIN)
    offsets = (jnp.cumsum(live_tiles) - live_tiles).astype(jnp.int32)
    rotation = jax.random.randint(key_turn, (), 0, N_BAND).astype(jnp.int32)
    tile_ids = jnp.arange(TILES_DEV, dtype=jnp.int32)
    global_tile = offsets[:, None] + tile_ids[None, :]
    dest_table = ((global_tile + rotation) % N_BAND).astype(jnp.int32)
    slot_table = jnp.where(tile_ids[None, :] < live_tiles[:, None], global_tile // N_BAND, CAP).astype(jnp.int32)
    return (keep_table, kept_windows, dest_table, slot_table)


def draw_keep_mask(key, part):
    return plan_tables(key)[0]


def draw_band_counts(key, part):
    return plan_tables(key)[1]


def draw_plan_dest(key, part):
    return plan_tables(key)[2]


def draw_plan_slot(key, part):
    return plan_tables(key)[3]


def draw_pixels(key, part):
    base_key = jax.random.fold_in(key, 201)
    values = jnp.clip(jax.random.normal(base_key, (HEIGHT, WIDTH, CHAN), jnp.float32), -6.0, 6.0)
    return values.astype(jnp.bfloat16)


def draw_qkv_weight(key, part):
    main_key = jax.random.fold_in(key, 301)
    weight = jax.random.normal(main_key, (CHAN, 3 * CHAN), jnp.float32) / math.sqrt(CHAN)
    return jnp.clip(weight, -5.0, 5.0).astype(jnp.bfloat16)


def noise(stream_key, shape, width, reach, kind=jnp.bfloat16):
    values = width * jax.random.normal(stream_key, shape, jnp.float32)
    return jnp.clip(values, min=-reach, max=reach).astype(kind)


def setup_inputs(seed: int = 0, part: int = 0) -> dict:
    seeds = jax.random.split(jax.random.key(seed), 13)
    part_keys = jax.random.split(jax.random.fold_in(seeds[12], part), 13)
    return {
        "pixels": draw_pixels(jax.random.fold_in(jax.random.fold_in(seeds[12], part), 71), part),
        "keep_mask": draw_keep_mask(jax.random.fold_in(jax.random.fold_in(seeds[12], part), 71), part),
        "band_counts": draw_band_counts(jax.random.fold_in(jax.random.fold_in(seeds[12], part), 71), part),
        "plan_dest": draw_plan_dest(jax.random.fold_in(jax.random.fold_in(seeds[12], part), 71), part),
        "plan_slot": draw_plan_slot(jax.random.fold_in(jax.random.fold_in(seeds[12], part), 71), part),
        "bias_table": noise(seeds[5], (TABLE, HEADS), 1.0, 4.0, jnp.float32),
        "gain_attn": jnp.clip(1.0 + 0.15 * jax.random.normal(seeds[6], (CHAN,), jnp.float32), 0.25, 1.75),
        "qkv_weight": draw_qkv_weight(jax.random.fold_in(seeds[12], 71), part),
        "proj_weight": noise(seeds[8], (CHAN, CHAN), CHAN ** -0.5, 0.4375),
        "gain_mlp": jnp.clip(1.0 + 0.15 * jax.random.normal(seeds[9], (CHAN,), jnp.float32), 0.25, 1.75),
        "hidden_weight": noise(seeds[10], (CHAN, FF_WIDTH), CHAN ** -0.5, 0.4375),
        "output_weight": noise(seeds[11], (FF_WIDTH, CHAN), FF_WIDTH ** -0.5, 0.3125),
    }


EPSILON = 1e-05

def layer_norm(values, gain_vec):
    values = values.astype(jnp.float32)
    center = values - lax.optimization_barrier(jnp.mean(values, axis=-1, keepdims=True))
    spread = lax.optimization_barrier(jnp.mean(center * center, axis=-1, keepdims=True))
    return center * lax.rsqrt(spread + EPSILON) * gain_vec

def position_bias(bias_table):
    coords = jnp.arange(WIN * WIN, dtype=jnp.int32)
    row_pos = coords // WIN
    col_pos = coords % WIN
    table_index = (row_pos[:, None] - row_pos[None, :] + WIN - 1) * (2 * WIN - 1) + (col_pos[:, None] - col_pos[None, :] + WIN - 1)
    return jnp.transpose(bias_table[table_index], (2, 0, 1))

def region_codes(first_row, row_count, height, col_count):
    rows_global = first_row + jnp.arange(row_count, dtype=jnp.int32)
    row_region = (rows_global >= height - WIN).astype(jnp.int32) + (rows_global >= height - SHIFT).astype(jnp.int32)
    col_global = jnp.arange(col_count, dtype=jnp.int32)
    col_region = (col_global >= col_count - WIN).astype(jnp.int32) + (col_global >= col_count - SHIFT).astype(jnp.int32)
    return 3 * row_region[:, None] + col_region[None, :]

def attend(windows, window_codes, head_bias, gain_attn, qkv_weight, proj_weight):
    window_count = windows.shape[0]
    head_dim = CHAN // HEADS
    normed = layer_norm(windows, gain_attn).astype(jnp.bfloat16).reshape(-1, CHAN)
    mixed_all = jnp.dot(normed, qkv_weight, preferred_element_type=jnp.float32).reshape(window_count, WIN * WIN, 3, HEADS, head_dim)
    queries = mixed_all[:, :, 0] * head_dim ** (-0.5)
    key_part = mixed_all[:, :, 1]
    value_part = lax.optimization_barrier(mixed_all[:, :, 2].astype(jnp.bfloat16)).astype(jnp.float32)
    scores = jnp.einsum('wqhd,wkhd->whqk', queries, key_part, precision=lax.Precision.HIGHEST)
    differ = window_codes[:, :, None] != window_codes[:, None, :]
    scores = scores + head_bias[None] + jnp.where(differ, -100.0, 0.0)[:, None]
    weights = jax.nn.softmax(scores, axis=-1).astype(jnp.bfloat16)
    weights = lax.optimization_barrier(weights).astype(jnp.float32)
    mixed = jnp.einsum('whqk,wkhd->wqhd', weights, value_part, precision=lax.Precision.HIGHEST)
    mixed = mixed.reshape(-1, CHAN).astype(jnp.bfloat16)
    projected = jnp.dot(mixed, proj_weight, preferred_element_type=jnp.float32)
    summed = windows.reshape(-1, CHAN).astype(jnp.float32) + projected
    return summed.astype(jnp.bfloat16).reshape(window_count, WIN * WIN, CHAN)

def feed(states, gain_mlp, hidden_weight, output_weight):
    flat_rows = states.reshape(-1, CHAN)
    normed = layer_norm(flat_rows, gain_mlp).astype(jnp.bfloat16)
    inner_act = jax.nn.gelu(jnp.dot(normed, hidden_weight, preferred_element_type=jnp.float32)).astype(jnp.bfloat16)
    summed = flat_rows.astype(jnp.float32) + jnp.dot(inner_act, output_weight, preferred_element_type=jnp.float32)
    return summed.astype(jnp.bfloat16).reshape(states.shape)

def reference(pixels, keep_mask, band_counts, plan_dest, plan_slot, bias_table, gain_attn, qkv_weight, proj_weight, gain_mlp, hidden_weight, output_weight):
    height = ROWS * N_BAND
    win_rows = ROWS // WIN
    win_cols = WIDTH // WIN
    shifted = jnp.roll(pixels, (-SHIFT, -SHIFT), axis=(0, 1))
    windows = shifted.reshape(N_BAND, win_rows, WIN, win_cols, WIN, CHAN).transpose(0, 1, 3, 2, 4, 5).reshape(N_BAND, WIN_DEV, WIN * WIN, CHAN)
    region_map = region_codes(0, height, height, WIDTH)
    window_codes = region_map.reshape(N_BAND, win_rows, WIN, win_cols, WIN).transpose(0, 1, 3, 2, 4).reshape(N_BAND, WIN_DEV, WIN * WIN)
    keep_rows = keep_mask.reshape(N_BAND, WIN_DEV)
    head_bias = position_bias(bias_table)

    def one_band(band_inputs):
        band_windows, band_codes, band_keep, band_count = band_inputs
        packed_order = (jnp.cumsum(band_keep) - 1).astype(jnp.int32)
        active = (band_keep == 1) & (packed_order < band_count)
        target = jnp.where(active, packed_order, WIN_DEV).astype(jnp.int32)
        packed = jnp.zeros((WIN_DEV + 1, WIN * WIN, CHAN), jnp.bfloat16).at[target].set(band_windows)[:WIN_DEV]
        packed_codes = jnp.zeros((WIN_DEV + 1, WIN * WIN), jnp.int32).at[target].set(band_codes)[:WIN_DEV]
        attended = attend(packed, packed_codes, head_bias, gain_attn, qkv_weight, proj_weight)
        finished = feed(attended, gain_mlp, hidden_weight, output_weight)
        unpacked = finished[jnp.clip(packed_order, 0, WIN_DEV - 1)]
        result = jnp.where(active[:, None, None], unpacked, band_windows)
        return (result, attended.reshape(TILES_DEV, TILE * WIN * WIN, CHAN))
    results, attended_all = lax.map(one_band, (windows, window_codes, keep_rows, band_counts))
    updated = results.reshape(N_BAND, win_rows, win_cols, WIN, WIN, CHAN).transpose(0, 1, 3, 2, 4, 5).reshape(height, WIDTH, CHAN)
    restored = jnp.roll(updated, (SHIFT, SHIFT), axis=(0, 1))
    tile_ids = jnp.arange(TILES_DEV, dtype=jnp.int32)
    tile_live = (tile_ids[None, :] * TILE < band_counts[:, None]) & (plan_slot < CAP)
    target = jnp.where(tile_live, plan_dest * CAP + plan_slot, N_BAND * CAP).astype(jnp.int32).reshape(-1)
    work_tiles = jnp.zeros((N_BAND * CAP + 1, TILE * WIN * WIN, CHAN), jnp.bfloat16)
    work_tiles = work_tiles.at[target].set(attended_all.reshape(-1, TILE * WIN * WIN, CHAN))[:N_BAND * CAP]
    return (restored, work_tiles)
```

```python
import functools

import jax
import jax.numpy as jnp
from jax import lax
from jax.experimental import pallas as pl
from jax.experimental.pallas import tpu as pltpu
from jax.sharding import PartitionSpec as P

CHAN = 180
HEADS = 6
WIN = 8
TILE = 2
SHIFT = 4
CAP = 8
TOK = WIN * WIN
HALF = TOK // 2
HEAD_DIM = CHAN // HEADS
HEAD_PAD = 32
GROUP = 4

EPSILON = 1e-05
BF = jnp.bfloat16
F32 = jnp.float32


def layer_norm(values, gain_vec):
    center = values - jnp.sum(values, axis=-1, keepdims=True) * (1.0 / CHAN)
    spread = jnp.sum(center * center, axis=-1, keepdims=True) * (1.0 / CHAN)
    return (center * lax.rsqrt(spread + EPSILON) * gain_vec).astype(BF)


def dot(a, b):
    return jnp.dot(a, b, preferred_element_type=F32)


def dot_t(a, b):
    return lax.dot_general(a, b, (((1,), (1,)), ((), ())), preferred_element_type=F32)


def biases(bias_ref, last_row, queries):
    first = TOK - queries
    parts = [bias_ref[h][:, first:] for h in range(HEADS)]
    base = jnp.concatenate(parts, axis=1)
    shape = (TOK, HEADS * queries)
    key = lax.broadcasted_iota(jnp.int32, shape, 0)
    query = lax.broadcasted_iota(jnp.int32, shape, 1) % queries + first
    rows_differ = (key // WIN >= SHIFT) != (query // WIN >= SHIFT)
    cols_differ = (key % WIN >= SHIFT) != (query % WIN >= SHIFT)
    row_pen = jnp.where(rows_differ, jnp.where(last_row, -100.0, 0.0).astype(F32), 0.0)
    plain = base + row_pen
    both = base + jnp.where(cols_differ, -100.0, row_pen)
    return plain, both


def attend(x, gain, wq, wk, wvt, wp, masks, eye, bias_of, queries):
    normed = layer_norm(x, gain)
    if queries == TOK:
        x_q, n_q = x, normed
    else:
        pick = lambda a: jnp.concatenate(
            [a[g * TOK + TOK - queries : (g + 1) * TOK] for g in range(GROUP)], axis=0
        )
        x_q, n_q = pick(x), pick(normed)
    q = (dot(n_q, wq) * HEAD_DIM ** (-0.5)).astype(BF)
    k = dot(normed, wk).astype(BF)
    vt = dot_t(wvt, normed).astype(BF)
    mixed = []
    for g in range(GROUP):
        q_w = q[g * queries : (g + 1) * queries]
        stacked = jnp.concatenate([q_w * masks[h] for h in range(HEADS)], axis=0)
        scores = dot_t(k[g * TOK : (g + 1) * TOK], stacked) + bias_of(g)
        top = jnp.max(scores, axis=0, keepdims=True)
        grown = jnp.exp(scores - top)
        weights = (grown * (1.0 / jnp.sum(grown, axis=0, keepdims=True))).astype(BF)
        v_w = vt[:, g * TOK : (g + 1) * TOK]
        heads = [
            dot(
                v_w[h * HEAD_PAD : (h + 1) * HEAD_PAD],
                weights[:, h * queries : (h + 1) * queries],
            )
            for h in range(HEADS)
        ]
        mixed.append(jnp.concatenate(heads, axis=0))
    mixed = jnp.concatenate(mixed, axis=1).astype(BF)
    count = GROUP * queries
    mixed = dot_t(eye[:count, :count], mixed).astype(BF)
    return (x_q + dot(mixed, wp)).astype(BF)


def feed(states, gain, wh, wo):
    flat = states.astype(F32)
    normed = layer_norm(flat, gain)
    inner = jax.nn.gelu(dot(normed, wh)).astype(BF)
    return (flat + dot(inner, wo)).astype(BF)


def roll_cols(x, by):
    by = by % x.shape[1]
    return jnp.concatenate([x[:, by:], x[:, :by]], axis=1)


def block_kernel(
    keep_own, keep_prev, counts, dests,
    pixels, nxt, prv, bias, gain_a, wq_r, wk_r, wvt_r, wp_r, gain_m, wh_r, wo_r,
    restored, outgoing,
    shifted, result, attended, bias_own, bias_prev, act_own, act_prev, order,
):
    bands = lax.axis_size("band")
    me = lax.axis_index("band")
    cols = pixels.shape[1]
    windows = cols // WIN
    tiles = windows // TILE
    pairs = -(-tiles // bands)

    def scan(w, carry):
        own, prev = carry
        a = (keep_own[w] == 1) & (own < counts[0])
        b = (keep_prev[w] == 1) & (prev < counts[1])
        act_own[w] = a.astype(jnp.int32)
        act_prev[w] = b.astype(jnp.int32)
        order[own] = w
        return own + keep_own[w], prev + keep_prev[w]

    own_total, _ = lax.fori_loop(0, windows, scan, (jnp.int32(0), jnp.int32(0)))
    live = jnp.minimum(own_total, counts[0])

    shifted[0:SHIFT] = roll_cols(prv[...].astype(F32), SHIFT)
    shifted[SHIFT : SHIFT + WIN] = roll_cols(pixels[...].astype(F32), SHIFT)
    shifted[SHIFT + WIN :] = roll_cols(nxt[...].astype(F32), SHIFT)

    bias_own[0], bias_own[1] = biases(bias, me == bands - 1, TOK)
    bias_prev[0], bias_prev[1] = biases(bias, me == 0, HALF)

    lane = lax.broadcasted_iota(jnp.int32, (1, CHAN), 1)
    masks = [
        ((lane >= h * HEAD_DIM) & (lane < (h + 1) * HEAD_DIM)).astype(F32).astype(BF)
        for h in range(HEADS)
    ]
    side = GROUP * TOK
    eye = (
        lax.broadcasted_iota(jnp.int32, (side, side), 0)
        == lax.broadcasted_iota(jnp.int32, (side, side), 1)
    ).astype(F32).astype(BF)

    def step(i, _):
        def load(row, g):
            start = pl.multiple_of((i * GROUP + g) * WIN, WIN)
            return shifted[row : row + WIN, pl.ds(start, WIN), :].reshape(TOK, CHAN)

        def edge(ref):
            return lambda g: ref[(i * GROUP + g == windows - 1).astype(jnp.int32)]

        weights = (gain_a[...], wq_r[...], wk_r[...], wvt_r[...], wp_r[...])
        x_own = jnp.concatenate([load(WIN, g) for g in range(GROUP)], axis=0)
        own = attend(x_own, *weights, masks, eye, edge(bias_own), TOK)
        for g in range(GROUP):
            attended[i * GROUP + g] = own[g * TOK : (g + 1) * TOK]
        x_prev = jnp.concatenate([load(0, g) for g in range(GROUP)], axis=0)
        prev = attend(x_prev, *weights, masks, eye, edge(bias_prev), HALF)
        upper = jnp.concatenate([own[g * TOK : g * TOK + HALF] for g in range(GROUP)] + [prev], axis=0)
        done = feed(upper, gain_m[...], wh_r[...], wo_r[...]).astype(F32)
        for g in range(GROUP):
            w = i * GROUP + g
            start = pl.multiple_of(w * WIN, WIN)
            upper_new = done[g * HALF : (g + 1) * HALF].reshape(SHIFT, WIN, CHAN)
            lower_new = done[(GROUP + g) * HALF : (GROUP + g + 1) * HALF].reshape(SHIFT, WIN, CHAN)
            upper_old = x_own[g * TOK : g * TOK + HALF].reshape(SHIFT, WIN, CHAN)
            lower_old = x_prev[g * TOK + HALF : (g + 1) * TOK].reshape(SHIFT, WIN, CHAN)
            result[0:SHIFT, pl.ds(start, WIN), :] = jnp.where(act_prev[w] == 1, lower_new, lower_old)
            result[SHIFT:, pl.ds(start, WIN), :] = jnp.where(act_own[w] == 1, upper_new, upper_old)
        return 0

    lax.fori_loop(0, windows // GROUP, step, 0)
    restored[...] = roll_cols(result[...], -SHIFT).astype(BF)

    def pack(t, _):
        place = dests[t] * pairs + t // bands
        for p in range(TILE):
            position = t * TILE + p
            valid = position < live
            source = order[jnp.minimum(position, jnp.maximum(live - 1, 0))]
            source = jnp.where(valid, source, 0)
            value = attended[source]
            outgoing[place, p * TOK : (p + 1) * TOK] = jnp.where(valid, value, jnp.zeros_like(value))
        return 0

    lax.fori_loop(0, tiles, pack, 0)


def prepare(bias_table, qkv_weight, proj_weight):
    coords = jnp.arange(TOK, dtype=jnp.int32)
    row_pos, col_pos = coords // WIN, coords % WIN
    key, query = (slice(None), None), (None, slice(None))
    index = (row_pos[query] - row_pos[key] + WIN - 1) * (2 * WIN - 1) + (
        col_pos[query] - col_pos[key] + WIN - 1
    )
    entries = bias_table.shape[0]
    onehot = (jnp.arange(entries, dtype=jnp.int32)[:, None] == index.reshape(1, -1)).astype(F32)
    bias = jnp.dot(bias_table.T, onehot, precision=lax.Precision.HIGHEST).reshape(HEADS, TOK, TOK)
    pad = ((0, 0), (0, HEAD_PAD - HEAD_DIM), (0, 0))
    wvt = qkv_weight[:, 2 * CHAN :].T.reshape(HEADS, HEAD_DIM, CHAN)
    wvt = jnp.pad(wvt, pad).reshape(HEADS * HEAD_PAD, CHAN)
    wp = jnp.pad(proj_weight.reshape(HEADS, HEAD_DIM, CHAN), pad).reshape(HEADS * HEAD_PAD, CHAN)
    return bias, qkv_weight[:, :CHAN], qkv_weight[:, CHAN : 2 * CHAN], wvt, wp


def shards(
    pixels, keep_mask, band_counts, plan_dest, plan_slot, bias_table, gain_attn, qkv_weight,
    proj_weight, gain_mlp, hidden_weight, output_weight,
):
    bands = lax.axis_size("band")
    me = lax.axis_index("band")
    rows, cols, channels = pixels.shape
    windows = cols // WIN
    tiles = windows // TILE
    pairs = -(-tiles // bands)
    ahead = [(s, (s + 1) % bands) for s in range(bands)]
    back = [(s, (s - 1) % bands) for s in range(bands)]
    nxt = lax.ppermute(pixels[:SHIFT], "band", back)
    prv = lax.ppermute(pixels[rows - SHIFT :], "band", ahead)

    live_slot = jnp.where(
        jnp.arange(tiles, dtype=jnp.int32) * TILE < band_counts[0], plan_slot[0], CAP
    )
    facts = jnp.concatenate([keep_mask[0], band_counts, plan_dest[0], live_slot])
    facts = lax.all_gather(facts, "band", axis=0, tiled=False)
    before = lax.dynamic_index_in_dim(facts, (me - 1) % bands, 0, keepdims=False)
    keep_prev = before[:windows]
    counts = jnp.stack([band_counts[0], before[windows]])
    all_dest = facts[:, windows + 1 : windows + 1 + tiles]
    all_slot = facts[:, windows + 1 + tiles :]
    arrives = jnp.arange(bands, dtype=jnp.int32)[:, None] * pairs + (
        jnp.arange(tiles, dtype=jnp.int32) // bands
    )
    hit = (all_dest == me)[None] & (all_slot[None] == jnp.arange(CAP, dtype=jnp.int32)[:, None, None])
    source = jnp.max(jnp.where(hit, arrives[None], -1), axis=(1, 2))

    bias, wq, wk, wvt, wp = prepare(bias_table, qkv_weight, proj_weight)
    smem = pl.BlockSpec(memory_space=pltpu.SMEM)
    vmem = pl.BlockSpec(memory_space=pltpu.VMEM)
    restored, outgoing = pl.pallas_call(
        block_kernel,
        out_shape=(
            jax.ShapeDtypeStruct((rows, cols, channels), BF),
            jax.ShapeDtypeStruct((bands * pairs, TILE * TOK, channels), BF),
        ),
        in_specs=[smem] * 4 + [vmem] * 12,
        out_specs=(vmem, vmem),
        scratch_shapes=[
            pltpu.VMEM((rows + 2 * SHIFT, cols, channels), F32),
            pltpu.VMEM((rows, cols, channels), F32),
            pltpu.VMEM((windows, TOK, channels), BF),
            pltpu.VMEM((2, TOK, HEADS * TOK), F32),
            pltpu.VMEM((2, TOK, HEADS * HALF), F32),
            pltpu.SMEM((windows,), jnp.int32),
            pltpu.SMEM((windows,), jnp.int32),
            pltpu.SMEM((windows + 1,), jnp.int32),
        ],
        compiler_params=pltpu.CompilerParams(vmem_limit_bytes=60 * 1024 * 1024),
        name="block",
    )(
        keep_mask[0], keep_prev, counts, plan_dest[0],
        pixels, nxt, prv, bias, gain_attn[None], wq, wk, wvt, wp, gain_mlp[None],
        hidden_weight, output_weight,
    )
    incoming = lax.all_to_all(
        outgoing.reshape(bands, pairs, TILE * TOK, channels), "band", split_axis=0, concat_axis=0, tiled=True
    ).reshape(bands * pairs, TILE * TOK, channels)
    picked = jnp.take(incoming, jnp.maximum(source, 0), axis=0)
    work = jnp.where((source >= 0)[:, None, None], picked, jnp.zeros_like(picked))
    return restored, work


def solution(mesh):
    split = P(("img", "band"))
    in_specs = (split,) * 5 + (P(),) * 7
    return jax.shard_map(shards, mesh=mesh, in_specs=in_specs, out_specs=(split, split), check_vma=False)
```

```python
import jax
import jax.numpy as jnp
from jax import lax
from jax.experimental import pallas as pl
from jax.experimental.pallas import tpu as pltpu
from jax.sharding import PartitionSpec as P

CHAN = 180
HEADS = 6
WIN = 8
TILE = 2
SHIFT = 4
CAP = 8
TOK = WIN * WIN
HALF = TOK // 2
HEAD_DIM = CHAN // HEADS
GROUP = 4
LANES = 128
SLOT_LANE = 120

EPSILON = 1e-05
BF = jnp.bfloat16
F32 = jnp.float32


def layer_norm(values, gain_vec):
    center = values - jnp.sum(values, axis=-1, keepdims=True) * (1.0 / CHAN)
    spread = jnp.sum(center * center, axis=-1, keepdims=True) * (1.0 / CHAN)
    return (center * lax.rsqrt(spread + EPSILON) * gain_vec).astype(BF)


def dot(a, b):
    return jnp.dot(a, b, preferred_element_type=F32)


def dot_t(a, b):
    return lax.dot_general(a, b, (((1,), (1,)), ((), ())), preferred_element_type=F32)


def biases(bias_ref, last_row, queries):
    first = TOK - queries
    base = jnp.concatenate([bias_ref[h][first:] for h in range(HEADS)], axis=0)
    shape = (HEADS * queries, TOK)
    key = lax.broadcasted_iota(jnp.int32, shape, 1)
    query = lax.broadcasted_iota(jnp.int32, shape, 0) % queries + first
    rows_differ = (key // WIN >= SHIFT) != (query // WIN >= SHIFT)
    cols_differ = (key % WIN >= SHIFT) != (query % WIN >= SHIFT)
    row_pen = jnp.where(rows_differ, jnp.where(last_row, -100.0, 0.0).astype(F32), 0.0)
    plain = base + row_pen
    both = base + jnp.where(cols_differ, -100.0, row_pen)
    return plain, both


def head_masks():
    lane = lax.broadcasted_iota(jnp.int32, (1, CHAN), 1)
    return [
        ((lane >= h * HEAD_DIM) & (lane < (h + 1) * HEAD_DIM)).astype(F32) for h in range(HEADS)
    ]


def attend(x, gain, wq, wk, wv, wp, bias_of, queries):
    masks = head_masks()
    low_masks = [m.astype(BF) for m in masks]
    normed = layer_norm(x, gain)
    if queries == TOK:
        x_q, n_q = x, normed
    else:
        pick = lambda a: jnp.concatenate(
            [a[g * TOK + TOK - queries : (g + 1) * TOK] for g in range(GROUP)], axis=0
        )
        x_q, n_q = pick(x), pick(normed)
    q = (dot(n_q, wq) * HEAD_DIM ** (-0.5)).astype(BF)
    k = dot(normed, wk).astype(BF)
    v = dot(normed, wv).astype(BF)
    mixed = []
    for g in range(GROUP):
        q_w = q[g * queries : (g + 1) * queries]
        stacked = jnp.concatenate([q_w * low_masks[h] for h in range(HEADS)], axis=0)
        scores = dot_t(stacked, k[g * TOK : (g + 1) * TOK]) + bias_of(g)
        top = jnp.max(scores, axis=1, keepdims=True)
        grown = jnp.exp(scores - top)
        weights = (grown * (1.0 / jnp.sum(grown, axis=1, keepdims=True))).astype(BF)
        wide = dot(weights, v[g * TOK : (g + 1) * TOK])
        total = wide[:queries] * masks[0]
        for h in range(1, HEADS):
            total = total + wide[h * queries : (h + 1) * queries] * masks[h]
        mixed.append(total)
    mixed = jnp.concatenate(mixed, axis=0).astype(BF)
    return (x_q + dot(mixed, wp)).astype(BF)


def feed(states, gain, wh, wo):
    flat = states.astype(F32)
    normed = layer_norm(flat, gain)
    inner = jax.nn.gelu(dot(normed, wh)).astype(BF)
    return (flat + dot(inner, wo)).astype(BF)


def roll_cols(x, by):
    by = by % x.shape[1]
    return jnp.concatenate([x[:, by:], x[:, :by]], axis=1)


def window_at(shifted, i, g, row):
    start = pl.multiple_of((i * GROUP + g) * WIN, WIN)
    return shifted[row : row + WIN, pl.ds(start, WIN), :].reshape(TOK, CHAN)


def group_at(shifted, i):
    return jnp.concatenate([window_at(shifted, i, g, 0) for g in range(GROUP)], axis=0)


def own_kernel(
    keep, count, dests, slots, pixels, nxt, bias, gain_a, wq, wk, wv, wp,
    upper, outgoing,
    shifted, first, rest, bias_own, order,
):
    bands = lax.axis_size("band")
    me = lax.axis_index("band")
    windows = pixels.shape[1] // WIN
    tiles = windows // TILE
    pairs = -(-tiles // bands)

    def scan(w, kept):
        order[kept] = w
        return kept + keep[w]

    live = jnp.minimum(lax.fori_loop(0, windows, scan, jnp.int32(0)), count[0])
    shifted[0 : WIN - SHIFT] = roll_cols(pixels[SHIFT:].astype(F32), SHIFT)
    shifted[WIN - SHIFT :] = roll_cols(nxt[...].astype(F32), SHIFT)
    bias_own[0], bias_own[1] = biases(bias, me == bands - 1, TOK)

    def step(i, _):
        def edge(g):
            return bias_own[(i * GROUP + g == windows - 1).astype(jnp.int32)]

        own = attend(group_at(shifted, i), gain_a[...], wq[...], wk[...], wv[...], wp[...], edge, TOK)
        for g in range(GROUP):
            w = i * GROUP + g
            value = own[g * TOK : (g + 1) * TOK]
            upper[w] = value[:HALF]
            first[w] = value[:, :LANES]
            rest[w, :, : CHAN - LANES] = value[:, LANES:].astype(F32)
        return 0

    lax.fori_loop(0, windows // GROUP, step, 0)
    if bands * pairs > tiles:
        outgoing[...] = jnp.full(outgoing.shape, CAP, BF)
    lane = lax.broadcasted_iota(jnp.int32, (TOK, LANES), 1)

    def pack(t, _):
        place = dests[t] * pairs + t // bands
        slot = jnp.where(t * TILE < live, slots[t], CAP).astype(F32)
        halves = []
        for p in range(TILE):
            position = t * TILE + p
            valid = position < live
            source = jnp.where(valid, order[jnp.where(valid, position, 0)], 0)
            value = first[source]
            outgoing[place, p * TOK : (p + 1) * TOK] = jnp.where(valid, value, jnp.zeros_like(value))
            tail = rest[source]
            halves.append(jnp.where(valid & (lane < CHAN - LANES), tail, 0.0))
        both = jnp.where(lane < TOK, halves[0], pltpu.roll(halves[1], TOK, 1))
        both = jnp.where(lane >= SLOT_LANE, slot, both)
        outgoing[place, TILE * TOK :] = both.astype(BF)
        return 0

    lax.fori_loop(0, tiles, pack, 0)


def map_kernel(
    keep_own, keep_prev, counts, pixels, prv, upper, bias, gain_a, wq, wk, wv, wp, gain_m, wh, wo,
    restored,
    shifted, result, bias_prev, act_own, act_prev,
):
    me = lax.axis_index("band")
    windows = pixels.shape[1] // WIN

    def scan(w, carry):
        own, prev = carry
        act_own[w] = ((keep_own[w] == 1) & (own < counts[0])).astype(jnp.int32)
        act_prev[w] = ((keep_prev[w] == 1) & (prev < counts[1])).astype(jnp.int32)
        return own + keep_own[w], prev + keep_prev[w]

    lax.fori_loop(0, windows, scan, (jnp.int32(0), jnp.int32(0)))
    shifted[0:SHIFT] = roll_cols(prv[...].astype(F32), SHIFT)
    shifted[SHIFT:] = roll_cols(pixels[...].astype(F32), SHIFT)
    bias_prev[0], bias_prev[1] = biases(bias, me == 0, HALF)

    def step(i, _):
        def edge(g):
            return bias_prev[(i * GROUP + g == windows - 1).astype(jnp.int32)]

        prev = attend(group_at(shifted, i), gain_a[...], wq[...], wk[...], wv[...], wp[...], edge, HALF)
        states = jnp.concatenate([upper[i * GROUP + g] for g in range(GROUP)] + [prev], axis=0)
        done = feed(states, gain_m[...], wh[...], wo[...]).astype(F32)
        for g in range(GROUP):
            w = i * GROUP + g
            cols = pl.ds(pl.multiple_of(w * WIN, WIN), WIN)
            upper_new = done[g * HALF : (g + 1) * HALF].reshape(SHIFT, WIN, CHAN)
            lower_new = done[(GROUP + g) * HALF : (GROUP + g + 1) * HALF].reshape(SHIFT, WIN, CHAN)
            result[0:SHIFT, cols, :] = jnp.where(
                act_prev[w] == 1, lower_new, shifted[SHIFT : 2 * SHIFT, cols, :]
            )
            result[SHIFT:, cols, :] = jnp.where(
                act_own[w] == 1, upper_new, shifted[2 * SHIFT :, cols, :]
            )
        return 0

    lax.fori_loop(0, windows // GROUP, step, 0)
    restored[...] = roll_cols(result[...], -SHIFT).astype(BF)


def place_kernel(incoming, work):
    work[...] = jnp.zeros(work.shape, BF)
    lane = lax.broadcasted_iota(jnp.int32, (16, LANES), 1)

    def put(t, _):
        head = incoming[t, TILE * TOK : TILE * TOK + 16].astype(F32)
        slot = jnp.max(jnp.where(lane >= SLOT_LANE, head, 0.0)).astype(jnp.int32)

        @pl.when(slot < CAP)
        def _():
            tail = incoming[t, TILE * TOK :].astype(F32)
            work[slot, :, :LANES] = incoming[t, : TILE * TOK]
            work[slot, :TOK, LANES:] = tail[:, : CHAN - LANES].astype(BF)
            work[slot, TOK:, LANES:] = pltpu.roll(tail, TOK, 1)[:, : CHAN - LANES].astype(BF)

        return 0

    lax.fori_loop(0, incoming.shape[0], put, 0)


def position_bias(bias_table):
    coords = jnp.arange(TOK, dtype=jnp.int32)
    row_pos, col_pos = coords // WIN, coords % WIN
    index = (row_pos[:, None] - row_pos[None, :] + WIN - 1) * (2 * WIN - 1) + (
        col_pos[:, None] - col_pos[None, :] + WIN - 1
    )
    entries = bias_table.shape[0]
    onehot = (jnp.arange(entries, dtype=jnp.int32)[:, None] == index.reshape(1, -1)).astype(F32)
    return jnp.dot(bias_table.T, onehot, precision=lax.Precision.HIGHEST).reshape(HEADS, TOK, TOK)


def shards(
    pixels, keep_mask, band_counts, plan_dest, plan_slot, bias_table, gain_attn, qkv_weight,
    proj_weight, gain_mlp, hidden_weight, output_weight,
):
    bands = lax.axis_size("band")
    rows, cols, channels = pixels.shape
    windows = cols // WIN
    tiles = windows // TILE
    pairs = -(-tiles // bands)
    ahead = [(s, (s + 1) % bands) for s in range(bands)]
    back = [(s, (s - 1) % bands) for s in range(bands)]
    turned = jnp.transpose(pixels, (2, 0, 1))
    nxt = jnp.transpose(lax.ppermute(turned[:, :SHIFT], "band", back), (1, 2, 0))
    prv = jnp.transpose(lax.ppermute(turned[:, rows - SHIFT :], "band", ahead), (1, 2, 0))
    facts = lax.ppermute(jnp.concatenate([keep_mask[0], band_counts]), "band", ahead)
    keep_prev = facts[:windows]
    counts = jnp.concatenate([band_counts, facts[windows:]])

    bias = position_bias(bias_table)
    wq, wk, wv = (qkv_weight[:, i * CHAN : (i + 1) * CHAN] for i in range(3))
    smem = pl.BlockSpec(memory_space=pltpu.SMEM)
    vmem = pl.BlockSpec(memory_space=pltpu.VMEM)
    limit = pltpu.CompilerParams(vmem_limit_bytes=40 * 1024 * 1024)
    upper, outgoing = pl.pallas_call(
        own_kernel,
        out_shape=(
            jax.ShapeDtypeStruct((windows, HALF, channels), BF),
            jax.ShapeDtypeStruct((bands * pairs, TILE * TOK + TOK, LANES), BF),
        ),
        in_specs=[smem] * 4 + [vmem] * 8,
        out_specs=(vmem, vmem),
        scratch_shapes=[
            pltpu.VMEM((rows, cols, channels), F32),
            pltpu.VMEM((windows, TOK, LANES), BF),
            pltpu.VMEM((windows, TOK, LANES), F32),
            pltpu.VMEM((2, HEADS * TOK, TOK), F32),
            pltpu.SMEM((windows + 1,), jnp.int32),
        ],
        compiler_params=limit,
        cost_estimate=pl.CostEstimate(flops=3 * 10**9, bytes_accessed=10**7, transcendentals=10**6),
        name="own",
    )(
        keep_mask[0], band_counts, plan_dest[0], plan_slot[0],
        pixels, nxt, bias, gain_attn[None], wq, wk, wv, proj_weight,
    )
    incoming = lax.all_to_all(
        outgoing.reshape(bands, -1, LANES), "band", split_axis=0, concat_axis=0, tiled=True
    ).reshape(outgoing.shape)
    restored = pl.pallas_call(
        map_kernel,
        out_shape=jax.ShapeDtypeStruct((rows, cols, channels), BF),
        in_specs=[smem] * 3 + [vmem] * 12,
        out_specs=vmem,
        scratch_shapes=[
            pltpu.VMEM((rows + SHIFT, cols, channels), F32),
            pltpu.VMEM((rows, cols, channels), F32),
            pltpu.VMEM((2, HEADS * HALF, TOK), F32),
            pltpu.SMEM((windows,), jnp.int32),
            pltpu.SMEM((windows,), jnp.int32),
        ],
        compiler_params=limit,
        cost_estimate=pl.CostEstimate(flops=10**10, bytes_accessed=3 * 10**7, transcendentals=10**6),
        name="map",
    )(
        keep_mask[0], keep_prev, counts, pixels, prv, upper, bias, gain_attn[None], wq, wk, wv,
        proj_weight, gain_mlp[None], hidden_weight, output_weight,
    )
    work = pl.pallas_call(
        place_kernel,
        out_shape=jax.ShapeDtypeStruct((CAP, TILE * TOK, channels), BF),
        in_specs=[vmem],
        out_specs=vmem,
        compiler_params=limit,
        name="place",
    )(incoming)
    return restored, work


def solution(mesh):
    split = P(("img", "band"))
    in_specs = (split,) * 5 + (P(),) * 7
    return jax.shard_map(shards, mesh=mesh, in_specs=in_specs, out_specs=(split, split), check_vma=False)
```

```python
import jax
import jax.numpy as jnp
from jax import lax
from jax.experimental import pallas as pl
from jax.experimental.pallas import tpu as pltpu
from jax.sharding import PartitionSpec as P

CHAN = 180
HEADS = 6
WIN = 8
TILE = 2
SHIFT = 4
CAP = 8
TOK = WIN * WIN
HALF = TOK // 2
HEAD_DIM = CHAN // HEADS
GROUP = 4
LANES = 128
SLOT_LANE = 120

EPSILON = 1e-05
BF = jnp.bfloat16
F32 = jnp.float32


def layer_norm(values, gain_vec):
    center = values - jnp.sum(values, axis=-1, keepdims=True) * (1.0 / CHAN)
    spread = jnp.sum(center * center, axis=-1, keepdims=True) * (1.0 / CHAN)
    return (center * lax.rsqrt(spread + EPSILON) * gain_vec).astype(BF)


def dot(a, b):
    return jnp.dot(a, b, preferred_element_type=F32)


def dot_t(a, b):
    return lax.dot_general(a, b, (((1,), (1,)), ((), ())), preferred_element_type=F32)


def biases(bias_ref, last_row, queries):
    first = TOK - queries
    base = jnp.concatenate([bias_ref[h][first:] for h in range(HEADS)], axis=0)
    shape = (HEADS * queries, TOK)
    key = lax.broadcasted_iota(jnp.int32, shape, 1)
    query = lax.broadcasted_iota(jnp.int32, shape, 0) % queries + first
    rows_differ = (key // WIN >= SHIFT) != (query // WIN >= SHIFT)
    cols_differ = (key % WIN >= SHIFT) != (query % WIN >= SHIFT)
    row_pen = jnp.where(rows_differ, jnp.where(last_row, -100.0, 0.0).astype(F32), 0.0)
    plain = base + row_pen
    both = base + jnp.where(cols_differ, -100.0, row_pen)
    return plain, both


def head_masks():
    lane = lax.broadcasted_iota(jnp.int32, (1, CHAN), 1)
    return [
        ((lane >= h * HEAD_DIM) & (lane < (h + 1) * HEAD_DIM)).astype(F32) for h in range(HEADS)
    ]


def attend(x, gain, wq, wk, wv, wp, bias_of, queries):
    masks = head_masks()
    low_masks = [m.astype(BF) for m in masks]
    normed = layer_norm(x, gain)
    if queries == TOK:
        x_q, n_q = x, normed
    else:
        pick = lambda a: jnp.concatenate(
            [a[g * TOK + TOK - queries : (g + 1) * TOK] for g in range(GROUP)], axis=0
        )
        x_q, n_q = pick(x), pick(normed)
    q = (dot(n_q, wq) * HEAD_DIM ** (-0.5)).astype(BF)
    k = dot(normed, wk).astype(BF)
    v = dot(normed, wv).astype(BF)
    mixed = []
    for g in range(GROUP):
        q_w = q[g * queries : (g + 1) * queries]
        stacked = jnp.concatenate([q_w * low_masks[h] for h in range(HEADS)], axis=0)
        scores = dot_t(stacked, k[g * TOK : (g + 1) * TOK]) + bias_of(g)
        top = jnp.max(scores, axis=1, keepdims=True)
        grown = jnp.exp(scores - top)
        weights = (grown * (1.0 / jnp.sum(grown, axis=1, keepdims=True))).astype(BF)
        wide = dot(weights, v[g * TOK : (g + 1) * TOK])
        total = wide[:queries] * masks[0]
        for h in range(1, HEADS):
            total = total + wide[h * queries : (h + 1) * queries] * masks[h]
        mixed.append(total)
    mixed = jnp.concatenate(mixed, axis=0).astype(BF)
    return (x_q + dot(mixed, wp)).astype(BF)


def feed(states, gain, wh, wo):
    flat = states.astype(F32)
    normed = layer_norm(flat, gain)
    inner = jax.nn.gelu(dot(normed, wh)).astype(BF)
    return (flat + dot(inner, wo)).astype(BF)


def roll_cols(x, by):
    by = by % x.shape[1]
    return jnp.concatenate([x[:, by:], x[:, :by]], axis=1)


def window_at(shifted, i, g, row):
    start = pl.multiple_of((i * GROUP + g) * WIN, WIN)
    return shifted[row : row + WIN, pl.ds(start, WIN), :].reshape(TOK, CHAN)


def group_at(shifted, i):
    return jnp.concatenate([window_at(shifted, i, g, 0) for g in range(GROUP)], axis=0)


def own_kernel(
    keep, count, dests, slots, pixels, nxt, bias, gain_a, wq, wk, wv, wp,
    upper, outgoing,
    shifted, first, rest, bias_own, order,
):
    bands = lax.axis_size("band")
    me = lax.axis_index("band")
    windows = pixels.shape[1] // WIN
    tiles = windows // TILE
    pairs = -(-tiles // bands)

    def scan(w, kept):
        order[kept] = w
        return kept + keep[w]

    live = jnp.minimum(lax.fori_loop(0, windows, scan, jnp.int32(0)), count[0])
    shifted[0 : WIN - SHIFT] = roll_cols(pixels[SHIFT:].astype(F32), SHIFT)
    shifted[WIN - SHIFT :] = roll_cols(nxt[...].astype(F32), SHIFT)
    bias_own[0], bias_own[1] = biases(bias, me == bands - 1, TOK)

    def step(i, _):
        def edge(g):
            return bias_own[(i * GROUP + g == windows - 1).astype(jnp.int32)]

        own = attend(group_at(shifted, i), gain_a[...], wq[...], wk[...], wv[...], wp[...], edge, TOK)
        for g in range(GROUP):
            w = i * GROUP + g
            value = own[g * TOK : (g + 1) * TOK]
            upper[w] = value[:HALF]
            first[w] = value[:, :LANES]
            rest[w, :, : CHAN - LANES] = value[:, LANES:].astype(F32)
        return 0

    lax.fori_loop(0, windows // GROUP, step, 0)
    if bands * pairs > tiles:
        outgoing[...] = jnp.full(outgoing.shape, CAP, BF)
    lane = lax.broadcasted_iota(jnp.int32, (TOK, LANES), 1)

    def pack(t, _):
        place = dests[t] * pairs + t // bands
        slot = jnp.where(t * TILE < live, slots[t], CAP).astype(F32)
        halves = []
        for p in range(TILE):
            position = t * TILE + p
            valid = position < live
            source = jnp.where(valid, order[jnp.where(valid, position, 0)], 0)
            value = first[source]
            outgoing[place, p * TOK : (p + 1) * TOK] = jnp.where(valid, value, jnp.zeros_like(value))
            tail = rest[source]
            halves.append(jnp.where(valid & (lane < CHAN - LANES), tail, 0.0))
        both = jnp.where(lane < TOK, halves[0], pltpu.roll(halves[1], TOK, 1))
        both = jnp.where(lane >= SLOT_LANE, slot, both)
        outgoing[place, TILE * TOK :] = both.astype(BF)
        return 0

    lax.fori_loop(0, tiles, pack, 0)


def map_kernel(
    keep_own, keep_prev, counts, pixels, prv, upper, bias, gain_a, wq, wk, wv, wp, gain_m, wh, wo,
    restored,
    shifted, result, bias_prev, act_own, act_prev,
):
    me = lax.axis_index("band")
    windows = pixels.shape[1] // WIN

    def scan(w, carry):
        own, prev = carry
        act_own[w] = ((keep_own[w] == 1) & (own < counts[0])).astype(jnp.int32)
        act_prev[w] = ((keep_prev[w] == 1) & (prev < counts[1])).astype(jnp.int32)
        return own + keep_own[w], prev + keep_prev[w]

    lax.fori_loop(0, windows, scan, (jnp.int32(0), jnp.int32(0)))
    shifted[0:SHIFT] = roll_cols(prv[...].astype(F32), SHIFT)
    shifted[SHIFT:] = roll_cols(pixels[...].astype(F32), SHIFT)
    bias_prev[0], bias_prev[1] = biases(bias, me == 0, HALF)

    def step(i, _):
        def edge(g):
            return bias_prev[(i * GROUP + g == windows - 1).astype(jnp.int32)]

        prev = attend(group_at(shifted, i), gain_a[...], wq[...], wk[...], wv[...], wp[...], edge, HALF)
        states = jnp.concatenate([upper[i * GROUP + g] for g in range(GROUP)] + [prev], axis=0)
        done = feed(states, gain_m[...], wh[...], wo[...]).astype(F32)
        for g in range(GROUP):
            w = i * GROUP + g
            cols = pl.ds(pl.multiple_of(w * WIN, WIN), WIN)
            upper_new = done[g * HALF : (g + 1) * HALF].reshape(SHIFT, WIN, CHAN)
            lower_new = done[(GROUP + g) * HALF : (GROUP + g + 1) * HALF].reshape(SHIFT, WIN, CHAN)
            result[0:SHIFT, cols, :] = jnp.where(
                act_prev[w] == 1, lower_new, shifted[SHIFT : 2 * SHIFT, cols, :]
            )
            result[SHIFT:, cols, :] = jnp.where(
                act_own[w] == 1, upper_new, shifted[2 * SHIFT :, cols, :]
            )
        return 0

    lax.fori_loop(0, windows // GROUP, step, 0)
    restored[...] = roll_cols(result[...], -SHIFT).astype(BF)


def place_kernel(incoming, work):
    work[...] = jnp.zeros(work.shape, BF)
    lane = lax.broadcasted_iota(jnp.int32, (16, LANES), 1)

    def put(t, _):
        head = incoming[t, TILE * TOK : TILE * TOK + 16].astype(F32)
        slot = jnp.max(jnp.where(lane >= SLOT_LANE, head, 0.0)).astype(jnp.int32)

        @pl.when(slot < CAP)
        def _():
            tail = incoming[t, TILE * TOK :].astype(F32)
            work[slot, :, :LANES] = incoming[t, : TILE * TOK]
            work[slot, :TOK, LANES:] = tail[:, : CHAN - LANES].astype(BF)
            work[slot, TOK:, LANES:] = pltpu.roll(tail, TOK, 1)[:, : CHAN - LANES].astype(BF)

        return 0

    lax.fori_loop(0, incoming.shape[0], put, 0)


def position_bias(bias_table):
    coords = jnp.arange(TOK, dtype=jnp.int32)
    row_pos, col_pos = coords // WIN, coords % WIN
    index = (row_pos[:, None] - row_pos[None, :] + WIN - 1) * (2 * WIN - 1) + (
        col_pos[:, None] - col_pos[None, :] + WIN - 1
    )
    entries = bias_table.shape[0]
    onehot = (jnp.arange(entries, dtype=jnp.int32)[:, None] == index.reshape(1, -1)).astype(F32)
    return jnp.dot(bias_table.T, onehot, precision=lax.Precision.HIGHEST).reshape(HEADS, TOK, TOK)


def shards(
    pixels, keep_mask, band_counts, plan_dest, plan_slot, bias_table, gain_attn, qkv_weight,
    proj_weight, gain_mlp, hidden_weight, output_weight,
):
    bands = lax.axis_size("band")
    rows, cols, channels = pixels.shape
    windows = cols // WIN
    tiles = windows // TILE
    pairs = -(-tiles // bands)
    ahead = [(s, (s + 1) % bands) for s in range(bands)]
    back = [(s, (s - 1) % bands) for s in range(bands)]
    turned = jnp.transpose(pixels, (2, 0, 1))
    nxt = jnp.transpose(lax.ppermute(turned[:, :SHIFT], "band", back), (1, 2, 0))
    prv = jnp.transpose(lax.ppermute(turned[:, rows - SHIFT :], "band", ahead), (1, 2, 0))
    facts = lax.ppermute(jnp.concatenate([keep_mask[0], band_counts]), "band", ahead)
    bias = position_bias(bias_table)
    nxt, prv, facts, bias = lax.optimization_barrier((nxt, prv, facts, bias))
    keep_prev = facts[:windows]
    counts = jnp.concatenate([band_counts, facts[windows:]])
    wq, wk, wv = (qkv_weight[:, i * CHAN : (i + 1) * CHAN] for i in range(3))
    smem = pl.BlockSpec(memory_space=pltpu.SMEM)
    vmem = pl.BlockSpec(memory_space=pltpu.VMEM)
    limit = pltpu.CompilerParams(vmem_limit_bytes=63 * 1024 * 1024)
    upper, outgoing = pl.pallas_call(
        own_kernel,
        out_shape=(
            jax.ShapeDtypeStruct((windows, HALF, channels), BF),
            jax.ShapeDtypeStruct((bands * pairs, TILE * TOK + TOK, LANES), BF),
        ),
        in_specs=[smem] * 4 + [vmem] * 8,
        out_specs=(vmem, vmem),
        scratch_shapes=[
            pltpu.VMEM((rows, cols, channels), F32),
            pltpu.VMEM((windows, TOK, LANES), BF),
            pltpu.VMEM((windows, TOK, LANES), F32),
            pltpu.VMEM((2, HEADS * TOK, TOK), F32),
            pltpu.SMEM((windows + 1,), jnp.int32),
        ],
        compiler_params=limit,
        cost_estimate=pl.CostEstimate(flops=3 * 10**9, bytes_accessed=10**7, transcendentals=10**6),
        name="own",
    )(
        keep_mask[0], band_counts, plan_dest[0], plan_slot[0],
        pixels, nxt, bias, gain_attn[None], wq, wk, wv, proj_weight,
    )
    incoming = lax.all_to_all(
        outgoing.reshape(bands, -1, LANES), "band", split_axis=0, concat_axis=0, tiled=True
    ).reshape(outgoing.shape)
    restored = pl.pallas_call(
        map_kernel,
        out_shape=jax.ShapeDtypeStruct((rows, cols, channels), BF),
        in_specs=[smem] * 3 + [vmem] * 12,
        out_specs=vmem,
        scratch_shapes=[
            pltpu.VMEM((rows + SHIFT, cols, channels), F32),
            pltpu.VMEM((rows, cols, channels), F32),
            pltpu.VMEM((2, HEADS * HALF, TOK), F32),
            pltpu.SMEM((windows,), jnp.int32),
            pltpu.SMEM((windows,), jnp.int32),
        ],
        compiler_params=limit,
        cost_estimate=pl.CostEstimate(flops=10**10, bytes_accessed=3 * 10**7, transcendentals=10**6),
        name="map",
    )(
        keep_mask[0], keep_prev, counts, pixels, prv, upper, bias, gain_attn[None], wq, wk, wv,
        proj_weight, gain_mlp[None], hidden_weight, output_weight,
    )
    work = pl.pallas_call(
        place_kernel,
        out_shape=jax.ShapeDtypeStruct((CAP, TILE * TOK, channels), BF),
        in_specs=[vmem],
        out_specs=vmem,
        compiler_params=limit,
        name="place",
    )(incoming)
    return restored, work


def solution(mesh):
    split = P(("img", "band"))
    in_specs = (split,) * 5 + (P(),) * 7
    return jax.shard_map(shards, mesh=mesh, in_specs=in_specs, out_specs=(split, split), check_vma=False)
```

```python
import jax
import jax.numpy as jnp
from jax import lax
from jax.experimental import pallas as pl
from jax.experimental.pallas import tpu as pltpu
from jax.sharding import PartitionSpec as P

CHAN = 180
HEADS = 6
WIN = 8
TILE = 2
SHIFT = 4
CAP = 8
TOK = WIN * WIN
HALF = TOK // 2
HEAD_DIM = CHAN // HEADS
GROUP = 4
LANES = 128
SLOT_LANE = 120

EPSILON = 1e-05
BF = jnp.bfloat16
F32 = jnp.float32


def layer_norm(values, gain_vec):
    center = values - jnp.sum(values, axis=-1, keepdims=True) * (1.0 / CHAN)
    spread = jnp.sum(center * center, axis=-1, keepdims=True) * (1.0 / CHAN)
    return (center * lax.rsqrt(spread + EPSILON) * gain_vec).astype(BF)


def dot(a, b):
    return jnp.dot(a, b, preferred_element_type=F32)


def dot_t(a, b):
    return lax.dot_general(a, b, (((1,), (1,)), ((), ())), preferred_element_type=F32)


def biases(bias_ref, last_row, queries):
    first = TOK - queries
    base = jnp.concatenate([bias_ref[h][first:] for h in range(HEADS)], axis=0)
    shape = (HEADS * queries, TOK)
    key = lax.broadcasted_iota(jnp.int32, shape, 1)
    query = lax.broadcasted_iota(jnp.int32, shape, 0) % queries + first
    rows_differ = (key // WIN >= SHIFT) != (query // WIN >= SHIFT)
    cols_differ = (key % WIN >= SHIFT) != (query % WIN >= SHIFT)
    row_pen = jnp.where(rows_differ, jnp.where(last_row, -100.0, 0.0).astype(F32), 0.0)
    plain = base + row_pen
    both = base + jnp.where(cols_differ, -100.0, row_pen)
    return plain, both


def head_masks():
    lane = lax.broadcasted_iota(jnp.int32, (1, CHAN), 1)
    return [
        ((lane >= h * HEAD_DIM) & (lane < (h + 1) * HEAD_DIM)).astype(F32) for h in range(HEADS)
    ]


def attend(x, gain, wq, wk, wv, wp, bias_of, queries):
    masks = head_masks()
    low_masks = [m.astype(BF) for m in masks]
    normed = layer_norm(x, gain)
    if queries == TOK:
        x_q, n_q = x, normed
    else:
        pick = lambda a: jnp.concatenate(
            [a[g * TOK + TOK - queries : (g + 1) * TOK] for g in range(GROUP)], axis=0
        )
        x_q, n_q = pick(x), pick(normed)
    q = (dot(n_q, wq) * HEAD_DIM ** (-0.5)).astype(BF)
    k = dot(normed, wk).astype(BF)
    v = dot(normed, wv).astype(BF)
    mixed = []
    for g in range(GROUP):
        q_w = q[g * queries : (g + 1) * queries]
        stacked = jnp.concatenate([q_w * low_masks[h] for h in range(HEADS)], axis=0)
        scores = dot_t(stacked, k[g * TOK : (g + 1) * TOK]) + bias_of(g)
        top = jnp.max(scores, axis=1, keepdims=True)
        grown = jnp.exp(scores - top)
        weights = (grown * (1.0 / jnp.sum(grown, axis=1, keepdims=True))).astype(BF)
        wide = dot(weights, v[g * TOK : (g + 1) * TOK])
        total = wide[:queries] * masks[0]
        for h in range(1, HEADS):
            total = total + wide[h * queries : (h + 1) * queries] * masks[h]
        mixed.append(total)
    mixed = jnp.concatenate(mixed, axis=0).astype(BF)
    return (x_q + dot(mixed, wp)).astype(BF)


def feed(states, gain, wh, wo):
    flat = states.astype(F32)
    normed = layer_norm(flat, gain)
    inner = jax.nn.gelu(dot(normed, wh)).astype(BF)
    return (flat + dot(inner, wo)).astype(BF)


def roll_cols(x, by):
    by = by % x.shape[1]
    return jnp.concatenate([x[:, by:], x[:, :by]], axis=1)


def window_at(shifted, i, g, row):
    start = pl.multiple_of((i * GROUP + g) * WIN, WIN)
    return shifted[row : row + WIN, pl.ds(start, WIN), :].reshape(TOK, CHAN)


def group_at(shifted, i):
    return jnp.concatenate([window_at(shifted, i, g, 0) for g in range(GROUP)], axis=0)


def own_kernel(
    pixels, bias, gain_a, wq, wk, wv, wp,
    upper, first, rest, prv,
    shifted, nxt_buf, prv_buf, bias_own, send_sem, recv_sem,
):
    bands = lax.axis_size("band")
    me = lax.axis_index("band")
    right, left = lax.rem(me + 1, bands), lax.rem(me + bands - 1, bands)
    rows, cols, _ = pixels.shape
    windows = cols // WIN
    groups = windows // GROUP
    chunks = groups // 2
    width = cols // chunks

    barrier = pltpu.get_barrier_semaphore()
    for neighbour in (left, right):
        pl.semaphore_signal(
            barrier, inc=1, device_id={"band": neighbour}, device_id_type=pl.DeviceIdType.MESH
        )
    pl.semaphore_wait(barrier, 2)
    copies = []
    for c in range(chunks):
        part = pl.ds(c * width, width)
        copies.append(
            pltpu.make_async_remote_copy(
                src_ref=pixels.at[0:SHIFT, part],
                dst_ref=nxt_buf.at[:, part],
                send_sem=send_sem.at[c],
                recv_sem=recv_sem.at[c],
                device_id={"band": left},
                device_id_type=pl.DeviceIdType.MESH,
            )
        )
    copies.append(
        pltpu.make_async_remote_copy(
            src_ref=pixels.at[rows - SHIFT : rows],
            dst_ref=prv_buf,
            send_sem=send_sem.at[chunks],
            recv_sem=recv_sem.at[chunks],
            device_id={"band": right},
            device_id_type=pl.DeviceIdType.MESH,
        )
    )
    for copy in copies:
        copy.start()

    shifted[0 : WIN - SHIFT] = roll_cols(pixels[SHIFT:].astype(F32), SHIFT)
    bias_own[0], bias_own[1] = biases(bias, me == bands - 1, TOK)

    def step(i, _):
        def edge(g):
            return bias_own[(i * GROUP + g == windows - 1).astype(jnp.int32)]

        own = attend(group_at(shifted, i), gain_a[...], wq[...], wk[...], wv[...], wp[...], edge, TOK)
        for g in range(GROUP):
            w = i * GROUP + g
            value = own[g * TOK : (g + 1) * TOK]
            upper[w] = value[:HALF]
            first[w] = value[:, :LANES]
            rest[w] = value[:, LANES:]
        return 0

    for c in range(chunks):
        copies[c].wait()
        low = c * width
        block = nxt_buf[:, low : low + width].astype(F32)
        if c == 0:
            shifted[WIN - SHIFT :, cols - SHIFT :] = block[:, :SHIFT]
            shifted[WIN - SHIFT :, 0 : width - SHIFT] = block[:, SHIFT:]
        else:
            shifted[WIN - SHIFT :, low - SHIFT : low + width - SHIFT] = block
        begin = 2 * c - 1 if c else 0
        end = 2 * c + 1 if c < chunks - 1 else groups
        lax.fori_loop(begin, end, step, 0)
    copies[chunks].wait()
    prv[...] = prv_buf[...]


def pack_kernel(keep, count, dests, slots, first, rest, outgoing, order):
    bands = lax.axis_size("band")
    windows = first.shape[0]
    tiles = windows // TILE
    pairs = -(-tiles // bands)

    def scan(w, kept):
        order[kept] = w
        return kept + keep[w]

    live = jnp.minimum(lax.fori_loop(0, windows, scan, jnp.int32(0)), count[0])
    if bands * pairs > tiles:
        outgoing[...] = jnp.full(outgoing.shape, CAP, BF)
    lane = lax.broadcasted_iota(jnp.int32, (TOK, LANES), 1)

    def pack(t, _):
        place = dests[t] * pairs + t // bands
        slot = jnp.where(t * TILE < live, slots[t], CAP).astype(F32)
        halves = []
        for p in range(TILE):
            position = t * TILE + p
            valid = position < live
            source = jnp.where(valid, order[jnp.where(valid, position, 0)], 0)
            value = first[source]
            outgoing[place, p * TOK : (p + 1) * TOK] = jnp.where(valid, value, jnp.zeros_like(value))
            tail = rest[source].astype(F32)
            tail = jnp.concatenate([tail, jnp.zeros((TOK, 2 * LANES - CHAN), F32)], axis=1)
            halves.append(jnp.where(valid, tail, 0.0))
        both = jnp.where(lane < TOK, halves[0], pltpu.roll(halves[1], TOK, 1))
        both = jnp.where(lane >= SLOT_LANE, slot, both)
        outgoing[place, TILE * TOK :] = both.astype(BF)
        return 0

    lax.fori_loop(0, tiles, pack, 0)


def map_kernel(
    keep_own, keep_prev, counts, pixels, prv, upper, bias, gain_a, wq, wk, wv, wp, gain_m, wh, wo,
    restored,
    shifted, result, bias_prev, act_own, act_prev,
):
    me = lax.axis_index("band")
    windows = pixels.shape[1] // WIN

    def scan(w, carry):
        own, prev = carry
        act_own[w] = ((keep_own[w] == 1) & (own < counts[0])).astype(jnp.int32)
        act_prev[w] = ((keep_prev[w] == 1) & (prev < counts[1])).astype(jnp.int32)
        return own + keep_own[w], prev + keep_prev[w]

    lax.fori_loop(0, windows, scan, (jnp.int32(0), jnp.int32(0)))
    shifted[0:SHIFT] = roll_cols(prv[...].astype(F32), SHIFT)
    shifted[SHIFT:] = roll_cols(pixels[...].astype(F32), SHIFT)
    bias_prev[0], bias_prev[1] = biases(bias, me == 0, HALF)

    def step(i, _):
        def edge(g):
            return bias_prev[(i * GROUP + g == windows - 1).astype(jnp.int32)]

        prev = attend(group_at(shifted, i), gain_a[...], wq[...], wk[...], wv[...], wp[...], edge, HALF)
        states = jnp.concatenate([upper[i * GROUP + g] for g in range(GROUP)] + [prev], axis=0)
        done = feed(states, gain_m[...], wh[...], wo[...]).astype(F32)
        for g in range(GROUP):
            w = i * GROUP + g
            cols = pl.ds(pl.multiple_of(w * WIN, WIN), WIN)
            upper_new = done[g * HALF : (g + 1) * HALF].reshape(SHIFT, WIN, CHAN)
            lower_new = done[(GROUP + g) * HALF : (GROUP + g + 1) * HALF].reshape(SHIFT, WIN, CHAN)
            result[0:SHIFT, cols, :] = jnp.where(
                act_prev[w] == 1, lower_new, shifted[SHIFT : 2 * SHIFT, cols, :]
            )
            result[SHIFT:, cols, :] = jnp.where(
                act_own[w] == 1, upper_new, shifted[2 * SHIFT :, cols, :]
            )
        return 0

    lax.fori_loop(0, windows // GROUP, step, 0)
    restored[...] = roll_cols(result[...], -SHIFT).astype(BF)


def place_kernel(incoming, work):
    work[...] = jnp.zeros(work.shape, BF)
    lane = lax.broadcasted_iota(jnp.int32, (16, LANES), 1)

    def put(t, _):
        head = incoming[t, TILE * TOK : TILE * TOK + 16].astype(F32)
        slot = jnp.max(jnp.where(lane >= SLOT_LANE, head, 0.0)).astype(jnp.int32)

        @pl.when(slot < CAP)
        def _():
            tail = incoming[t, TILE * TOK :].astype(F32)
            work[slot, :, :LANES] = incoming[t, : TILE * TOK]
            work[slot, :TOK, LANES:] = tail[:, : CHAN - LANES].astype(BF)
            work[slot, TOK:, LANES:] = pltpu.roll(tail, TOK, 1)[:, : CHAN - LANES].astype(BF)

        return 0

    lax.fori_loop(0, incoming.shape[0], put, 0)


def position_bias(bias_table):
    coords = jnp.arange(TOK, dtype=jnp.int32)
    row_pos, col_pos = coords // WIN, coords % WIN
    index = (row_pos[:, None] - row_pos[None, :] + WIN - 1) * (2 * WIN - 1) + (
        col_pos[:, None] - col_pos[None, :] + WIN - 1
    )
    entries = bias_table.shape[0]
    onehot = (jnp.arange(entries, dtype=jnp.int32)[:, None] == index.reshape(1, -1)).astype(F32)
    return jnp.dot(bias_table.T, onehot, precision=lax.Precision.HIGHEST).reshape(HEADS, TOK, TOK)


def shards(
    pixels, keep_mask, band_counts, plan_dest, plan_slot, bias_table, gain_attn, qkv_weight,
    proj_weight, gain_mlp, hidden_weight, output_weight,
):
    bands = lax.axis_size("band")
    rows, cols, channels = pixels.shape
    windows = cols // WIN
    tiles = windows // TILE
    pairs = -(-tiles // bands)
    ahead = [(s, (s + 1) % bands) for s in range(bands)]
    facts = lax.ppermute(jnp.concatenate([keep_mask[0], band_counts]), "band", ahead)
    bias = position_bias(bias_table)
    facts, bias = lax.optimization_barrier((facts, bias))
    keep_prev = facts[:windows]
    counts = jnp.concatenate([band_counts, facts[windows:]])
    wq, wk, wv = (qkv_weight[:, i * CHAN : (i + 1) * CHAN] for i in range(3))
    smem = pl.BlockSpec(memory_space=pltpu.SMEM)
    vmem = pl.BlockSpec(memory_space=pltpu.VMEM)
    limit = pltpu.CompilerParams(vmem_limit_bytes=63 * 1024 * 1024)
    chunks = windows // GROUP // 2
    upper, first, rest, prv = pl.pallas_call(
        own_kernel,
        out_shape=(
            jax.ShapeDtypeStruct((windows, HALF, channels), BF),
            jax.ShapeDtypeStruct((windows, TOK, LANES), BF),
            jax.ShapeDtypeStruct((windows, TOK, channels - LANES), BF),
            jax.ShapeDtypeStruct((SHIFT, cols, channels), BF),
        ),
        in_specs=[vmem] * 7,
        out_specs=(vmem,) * 4,
        scratch_shapes=[
            pltpu.VMEM((rows, cols, channels), F32),
            pltpu.VMEM((SHIFT, cols, channels), BF),
            pltpu.VMEM((SHIFT, cols, channels), BF),
            pltpu.VMEM((2, HEADS * TOK, TOK), F32),
            pltpu.SemaphoreType.DMA((chunks + 1,)),
            pltpu.SemaphoreType.DMA((chunks + 1,)),
        ],
        compiler_params=pltpu.CompilerParams(
            vmem_limit_bytes=63 * 1024 * 1024, collective_id=0, has_side_effects=True
        ),
        cost_estimate=pl.CostEstimate(flops=3 * 10**9, bytes_accessed=10**7, transcendentals=10**6),
        name="own",
    )(pixels, bias, gain_attn[None], wq, wk, wv, proj_weight)
    outgoing = pl.pallas_call(
        pack_kernel,
        out_shape=jax.ShapeDtypeStruct((bands * pairs, TILE * TOK + TOK, LANES), BF),
        in_specs=[smem] * 4 + [vmem] * 2,
        out_specs=vmem,
        scratch_shapes=[pltpu.SMEM((windows + 1,), jnp.int32)],
        compiler_params=limit,
        name="pack",
    )(keep_mask[0], band_counts, plan_dest[0], plan_slot[0], first, rest)
    incoming = lax.all_to_all(
        outgoing.reshape(bands, -1, LANES), "band", split_axis=0, concat_axis=0, tiled=True
    ).reshape(outgoing.shape)
    restored = pl.pallas_call(
        map_kernel,
        out_shape=jax.ShapeDtypeStruct((rows, cols, channels), BF),
        in_specs=[smem] * 3 + [vmem] * 12,
        out_specs=vmem,
        scratch_shapes=[
            pltpu.VMEM((rows + SHIFT, cols, channels), F32),
            pltpu.VMEM((rows, cols, channels), F32),
            pltpu.VMEM((2, HEADS * HALF, TOK), F32),
            pltpu.SMEM((windows,), jnp.int32),
            pltpu.SMEM((windows,), jnp.int32),
        ],
        compiler_params=limit,
        cost_estimate=pl.CostEstimate(flops=10**10, bytes_accessed=3 * 10**7, transcendentals=10**6),
        name="map",
    )(
        keep_mask[0], keep_prev, counts, pixels, prv, upper, bias, gain_attn[None], wq, wk, wv,
        proj_weight, gain_mlp[None], hidden_weight, output_weight,
    )
    work = pl.pallas_call(
        place_kernel,
        out_shape=jax.ShapeDtypeStruct((CAP, TILE * TOK, channels), BF),
        in_specs=[vmem],
        out_specs=vmem,
        compiler_params=limit,
        name="place",
    )(incoming)
    return restored, work


def solution(mesh):
    split = P(("img", "band"))
    in_specs = (split,) * 5 + (P(),) * 7
    return jax.shard_map(shards, mesh=mesh, in_specs=in_specs, out_specs=(split, split), check_vma=False)
```

```python
import jax
import jax.numpy as jnp
from jax import lax
from jax.experimental import pallas as pl
from jax.experimental.pallas import tpu as pltpu
from jax.sharding import PartitionSpec as P

CHAN = 180
HEADS = 6
WIN = 8
TILE = 2
SHIFT = 4
CAP = 8
TOK = WIN * WIN
HALF = TOK // 2
HEAD_DIM = CHAN // HEADS
GROUP = 4
LANES = 128
SLOT_LANE = 120

EPSILON = 1e-05
BF = jnp.bfloat16
F32 = jnp.float32


def layer_norm(values, gain_vec):
    center = values - jnp.sum(values, axis=-1, keepdims=True) * (1.0 / CHAN)
    spread = jnp.sum(center * center, axis=-1, keepdims=True) * (1.0 / CHAN)
    return (center * lax.rsqrt(spread + EPSILON) * gain_vec).astype(BF)


def dot(a, b):
    return jnp.dot(a, b, preferred_element_type=F32)


def dot_t(a, b):
    return lax.dot_general(a, b, (((1,), (1,)), ((), ())), preferred_element_type=F32)


def biases(bias_ref, last_row, queries):
    first = TOK - queries
    base = jnp.concatenate([bias_ref[h][first:] for h in range(HEADS)], axis=0)
    shape = (HEADS * queries, TOK)
    key = lax.broadcasted_iota(jnp.int32, shape, 1)
    query = lax.broadcasted_iota(jnp.int32, shape, 0) % queries + first
    rows_differ = (key // WIN >= SHIFT) != (query // WIN >= SHIFT)
    cols_differ = (key % WIN >= SHIFT) != (query % WIN >= SHIFT)
    row_pen = jnp.where(rows_differ, jnp.where(last_row, -100.0, 0.0).astype(F32), 0.0)
    plain = base + row_pen
    both = base + jnp.where(cols_differ, -100.0, row_pen)
    return plain, both


def head_masks():
    lane = lax.broadcasted_iota(jnp.int32, (1, CHAN), 1)
    return [
        ((lane >= h * HEAD_DIM) & (lane < (h + 1) * HEAD_DIM)).astype(F32) for h in range(HEADS)
    ]


def attend(x, gain, wq, wk, wv, wp, bias_of, queries):
    masks = head_masks()
    low_masks = [m.astype(BF) for m in masks]
    normed = layer_norm(x, gain)
    if queries == TOK:
        x_q, n_q = x, normed
    else:
        pick = lambda a: jnp.concatenate(
            [a[g * TOK + TOK - queries : (g + 1) * TOK] for g in range(GROUP)], axis=0
        )
        x_q, n_q = pick(x), pick(normed)
    q = (dot(n_q, wq) * HEAD_DIM ** (-0.5)).astype(BF)
    k = dot(normed, wk).astype(BF)
    v = dot(normed, wv).astype(BF)
    mixed = []
    for g in range(GROUP):
        q_w = q[g * queries : (g + 1) * queries]
        stacked = jnp.concatenate([q_w * low_masks[h] for h in range(HEADS)], axis=0)
        scores = dot_t(stacked, k[g * TOK : (g + 1) * TOK]) + bias_of(g)
        top = jnp.max(scores, axis=1, keepdims=True)
        grown = jnp.exp(scores - top)
        weights = (grown * (1.0 / jnp.sum(grown, axis=1, keepdims=True))).astype(BF)
        wide = dot(weights, v[g * TOK : (g + 1) * TOK])
        total = wide[:queries] * masks[0]
        for h in range(1, HEADS):
            total = total + wide[h * queries : (h + 1) * queries] * masks[h]
        mixed.append(total)
    mixed = jnp.concatenate(mixed, axis=0).astype(BF)
    return (x_q + dot(mixed, wp)).astype(BF)


def feed(states, gain, wh, wo):
    flat = states.astype(F32)
    normed = layer_norm(flat, gain)
    inner = jax.nn.gelu(dot(normed, wh)).astype(BF)
    return (flat + dot_t(inner, wo)).astype(BF)


def roll_cols(x, by):
    by = by % x.shape[1]
    return jnp.concatenate([x[:, by:], x[:, :by]], axis=1)


def window_at(shifted, i, g, row):
    start = pl.multiple_of((i * GROUP + g) * WIN, WIN)
    return shifted[row : row + WIN, pl.ds(start, WIN), :].reshape(TOK, CHAN)


def group_at(shifted, i):
    return jnp.concatenate([window_at(shifted, i, g, 0) for g in range(GROUP)], axis=0)


def own_kernel(
    pixels, bias, gain_a, wq, wk, wv, wp,
    upper, first, rest, prv,
    shifted, nxt_buf, prv_buf, bias_own, send_sem, recv_sem,
):
    bands = lax.axis_size("band")
    me = lax.axis_index("band")
    right, left = lax.rem(me + 1, bands), lax.rem(me + bands - 1, bands)
    rows, cols, _ = pixels.shape
    windows = cols // WIN
    groups = windows // GROUP
    chunks = groups // 2
    width = cols // chunks

    barrier = pltpu.get_barrier_semaphore()
    for neighbour in (left, right):
        pl.semaphore_signal(
            barrier, inc=1, device_id={"band": neighbour}, device_id_type=pl.DeviceIdType.MESH
        )
    pl.semaphore_wait(barrier, 2)
    copies = []
    for c in range(chunks):
        part = pl.ds(c * width, width)
        copies.append(
            pltpu.make_async_remote_copy(
                src_ref=pixels.at[0:SHIFT, part],
                dst_ref=nxt_buf.at[:, part],
                send_sem=send_sem.at[c],
                recv_sem=recv_sem.at[c],
                device_id={"band": left},
                device_id_type=pl.DeviceIdType.MESH,
            )
        )
    copies.append(
        pltpu.make_async_remote_copy(
            src_ref=pixels.at[rows - SHIFT : rows],
            dst_ref=prv_buf,
            send_sem=send_sem.at[chunks],
            recv_sem=recv_sem.at[chunks],
            device_id={"band": right},
            device_id_type=pl.DeviceIdType.MESH,
        )
    )
    for copy in copies[:chunks]:
        copy.start()

    shifted[0 : WIN - SHIFT] = roll_cols(pixels[SHIFT:].astype(F32), SHIFT)
    bias_own[0], bias_own[1] = biases(bias, me == bands - 1, TOK)

    def step(i, _):
        def edge(g):
            return bias_own[(i * GROUP + g == windows - 1).astype(jnp.int32)]

        own = attend(group_at(shifted, i), gain_a[...], wq[...], wk[...], wv[...], wp[...], edge, TOK)
        for g in range(GROUP):
            w = i * GROUP + g
            value = own[g * TOK : (g + 1) * TOK]
            upper[w] = value[:HALF]
            first[w] = value[:, :LANES]
            rest[w] = value[:, LANES:]
        return 0

    for c in range(chunks):
        copies[c].wait()
        if c == chunks // 2:
            copies[chunks].start()
        low = c * width
        block = nxt_buf[:, low : low + width].astype(F32)
        if c == 0:
            shifted[WIN - SHIFT :, cols - SHIFT :] = block[:, :SHIFT]
            shifted[WIN - SHIFT :, 0 : width - SHIFT] = block[:, SHIFT:]
        else:
            shifted[WIN - SHIFT :, low - SHIFT : low + width - SHIFT] = block
        begin = 2 * c - 1 if c else 0
        end = 2 * c + 1 if c < chunks - 1 else groups
        lax.fori_loop(begin, end, step, 0)
    copies[chunks].wait()
    prv[...] = prv_buf[...]


def pack_kernel(keep, count, dests, slots, first, rest, outgoing, order):
    bands = lax.axis_size("band")
    windows = first.shape[0]
    tiles = windows // TILE
    pairs = -(-tiles // bands)

    def scan(w, kept):
        order[kept] = w
        return kept + keep[w]

    live = jnp.minimum(lax.fori_loop(0, windows, scan, jnp.int32(0)), count[0])
    if bands * pairs > tiles:
        outgoing[...] = jnp.full(outgoing.shape, CAP, BF)
    lane = lax.broadcasted_iota(jnp.int32, (TOK, LANES), 1)

    def pack(t, _):
        place = dests[t] * pairs + t // bands
        slot = jnp.where(t * TILE < live, slots[t], CAP).astype(F32)
        halves = []
        for p in range(TILE):
            position = t * TILE + p
            valid = position < live
            source = jnp.where(valid, order[jnp.where(valid, position, 0)], 0)
            value = first[source]
            outgoing[place, p * TOK : (p + 1) * TOK] = jnp.where(valid, value, jnp.zeros_like(value))
            tail = rest[source].astype(F32)
            tail = jnp.concatenate([tail, jnp.zeros((TOK, 2 * LANES - CHAN), F32)], axis=1)
            halves.append(jnp.where(valid, tail, 0.0))
        both = jnp.where(lane < TOK, halves[0], pltpu.roll(halves[1], TOK, 1))
        both = jnp.where(lane >= SLOT_LANE, slot, both)
        outgoing[place, TILE * TOK :] = both.astype(BF)
        return 0

    lax.fori_loop(0, tiles, pack, 0)


def map_kernel(
    keep_own, count, facts, pixels, prv, upper, bias, gain_a, wq, wk, wv, wp, gain_m, wh, wo,
    restored,
    shifted, result, bias_prev, act_own, act_prev,
):
    me = lax.axis_index("band")
    windows = pixels.shape[1] // WIN

    def scan(w, carry):
        own, prev = carry
        act_own[w] = ((keep_own[w] == 1) & (own < count[0])).astype(jnp.int32)
        act_prev[w] = ((facts[w] == 1) & (prev < facts[windows])).astype(jnp.int32)
        return own + keep_own[w], prev + facts[w]

    lax.fori_loop(0, windows, scan, (jnp.int32(0), jnp.int32(0)))
    shifted[0:SHIFT] = roll_cols(prv[...].astype(F32), SHIFT)
    shifted[SHIFT:] = roll_cols(pixels[...].astype(F32), SHIFT)
    bias_prev[0], bias_prev[1] = biases(bias, me == 0, HALF)

    def step(i, _):
        def edge(g):
            return bias_prev[(i * GROUP + g == windows - 1).astype(jnp.int32)]

        prev = attend(group_at(shifted, i), gain_a[...], wq[...], wk[...], wv[...], wp[...], edge, HALF)
        states = jnp.concatenate([upper[i * GROUP + g] for g in range(GROUP)] + [prev], axis=0)
        done = feed(states, gain_m[...], wh[...], wo[...]).astype(F32)
        for g in range(GROUP):
            w = i * GROUP + g
            cols = pl.ds(pl.multiple_of(w * WIN, WIN), WIN)
            upper_new = done[g * HALF : (g + 1) * HALF].reshape(SHIFT, WIN, CHAN)
            lower_new = done[(GROUP + g) * HALF : (GROUP + g + 1) * HALF].reshape(SHIFT, WIN, CHAN)
            result[0:SHIFT, cols, :] = jnp.where(
                act_prev[w] == 1, lower_new, shifted[SHIFT : 2 * SHIFT, cols, :]
            )
            result[SHIFT:, cols, :] = jnp.where(
                act_own[w] == 1, upper_new, shifted[2 * SHIFT :, cols, :]
            )
        return 0

    lax.fori_loop(0, windows // GROUP, step, 0)
    restored[...] = roll_cols(result[...], -SHIFT).astype(BF)


def place_kernel(incoming, work):
    work[...] = jnp.zeros(work.shape, BF)
    lane = lax.broadcasted_iota(jnp.int32, (16, LANES), 1)

    def put(t, _):
        head = incoming[t, TILE * TOK : TILE * TOK + 16].astype(F32)
        slot = jnp.max(jnp.where(lane >= SLOT_LANE, head, 0.0)).astype(jnp.int32)

        @pl.when(slot < CAP)
        def _():
            tail = incoming[t, TILE * TOK :].astype(F32)
            work[slot, :, :LANES] = incoming[t, : TILE * TOK]
            work[slot, :TOK, LANES:] = tail[:, : CHAN - LANES].astype(BF)
            work[slot, TOK:, LANES:] = pltpu.roll(tail, TOK, 1)[:, : CHAN - LANES].astype(BF)

        return 0

    lax.fori_loop(0, incoming.shape[0], put, 0)


def position_bias(bias_table):
    coords = jnp.arange(TOK, dtype=jnp.int32)
    row_pos, col_pos = coords // WIN, coords % WIN
    index = (row_pos[:, None] - row_pos[None, :] + WIN - 1) * (2 * WIN - 1) + (
        col_pos[:, None] - col_pos[None, :] + WIN - 1
    )
    entries = bias_table.shape[0]
    onehot = (jnp.arange(entries, dtype=jnp.int32)[:, None] == index.reshape(1, -1)).astype(F32)
    return jnp.dot(bias_table.T, onehot, precision=lax.Precision.HIGHEST).reshape(HEADS, TOK, TOK)


def shards(
    pixels, keep_mask, band_counts, plan_dest, plan_slot, bias_table, gain_attn, qkv_weight,
    proj_weight, gain_mlp, hidden_weight, output_weight,
):
    bands = lax.axis_size("band")
    rows, cols, channels = pixels.shape
    windows = cols // WIN
    tiles = windows // TILE
    pairs = -(-tiles // bands)
    ahead = [(s, (s + 1) % bands) for s in range(bands)]
    facts = lax.ppermute(jnp.concatenate([keep_mask[0], band_counts]), "band", ahead)
    bias = position_bias(bias_table)
    facts, bias = lax.optimization_barrier((facts, bias))
    wq, wk, wv = (qkv_weight[:, i * CHAN : (i + 1) * CHAN] for i in range(3))
    smem = pl.BlockSpec(memory_space=pltpu.SMEM)
    vmem = pl.BlockSpec(memory_space=pltpu.VMEM)
    limit = pltpu.CompilerParams(vmem_limit_bytes=63 * 1024 * 1024)
    chunks = windows // GROUP // 2
    upper, first, rest, prv = pl.pallas_call(
        own_kernel,
        out_shape=(
            jax.ShapeDtypeStruct((windows, HALF, channels), BF),
            jax.ShapeDtypeStruct((windows, TOK, LANES), BF),
            jax.ShapeDtypeStruct((windows, TOK, channels - LANES), BF),
            jax.ShapeDtypeStruct((SHIFT, cols, channels), BF),
        ),
        in_specs=[vmem] * 7,
        out_specs=(vmem,) * 4,
        scratch_shapes=[
            pltpu.VMEM((rows, cols, channels), F32),
            pltpu.VMEM((SHIFT, cols, channels), BF),
            pltpu.VMEM((SHIFT, cols, channels), BF),
            pltpu.VMEM((2, HEADS * TOK, TOK), F32),
            pltpu.SemaphoreType.DMA((chunks + 1,)),
            pltpu.SemaphoreType.DMA((chunks + 1,)),
        ],
        compiler_params=pltpu.CompilerParams(
            vmem_limit_bytes=63 * 1024 * 1024, collective_id=0, has_side_effects=True
        ),
        cost_estimate=pl.CostEstimate(flops=3 * 10**9, bytes_accessed=10**7, transcendentals=10**6),
        name="own",
    )(pixels, bias, gain_attn[None], wq, wk, wv, proj_weight)
    outgoing = pl.pallas_call(
        pack_kernel,
        out_shape=jax.ShapeDtypeStruct((bands * pairs, TILE * TOK + TOK, LANES), BF),
        in_specs=[smem] * 4 + [vmem] * 2,
        out_specs=vmem,
        scratch_shapes=[pltpu.SMEM((windows + 1,), jnp.int32)],
        compiler_params=limit,
        name="pack",
    )(keep_mask[0], band_counts, plan_dest[0], plan_slot[0], first, rest)
    incoming = lax.all_to_all(
        outgoing.reshape(bands, -1, LANES), "band", split_axis=0, concat_axis=0, tiled=True
    ).reshape(outgoing.shape)
    restored = pl.pallas_call(
        map_kernel,
        out_shape=jax.ShapeDtypeStruct((rows, cols, channels), BF),
        in_specs=[smem] * 3 + [vmem] * 12,
        out_specs=vmem,
        scratch_shapes=[
            pltpu.VMEM((rows + SHIFT, cols, channels), F32),
            pltpu.VMEM((rows, cols, channels), F32),
            pltpu.VMEM((2, HEADS * HALF, TOK), F32),
            pltpu.SMEM((windows,), jnp.int32),
            pltpu.SMEM((windows,), jnp.int32),
        ],
        compiler_params=limit,
        cost_estimate=pl.CostEstimate(flops=10**10, bytes_accessed=3 * 10**7, transcendentals=10**6),
        name="map",
    )(
        keep_mask[0], band_counts, facts, pixels, prv, upper, bias, gain_attn[None], wq, wk, wv,
        proj_weight, gain_mlp[None], hidden_weight, output_weight.T,
    )
    work = pl.pallas_call(
        place_kernel,
        out_shape=jax.ShapeDtypeStruct((CAP, TILE * TOK, channels), BF),
        in_specs=[vmem],
        out_specs=vmem,
        compiler_params=pltpu.CompilerParams(vmem_limit_bytes=16 * 1024 * 1024),
        name="place",
    )(incoming)
    return restored, work


def solution(mesh):
    split = P(("img", "band"))
    in_specs = (split,) * 5 + (P(),) * 7
    return jax.shard_map(shards, mesh=mesh, in_specs=in_specs, out_specs=(split, split), check_vma=False)
```

```python
import jax
import jax.numpy as jnp
from jax import lax
from jax.experimental import pallas as pl
from jax.experimental.pallas import tpu as pltpu
from jax.sharding import PartitionSpec as P

CHAN = 180
HEADS = 6
WIN = 8
TILE = 2
SHIFT = 4
CAP = 8
TOK = WIN * WIN
HALF = TOK // 2
HEAD_DIM = CHAN // HEADS
GROUP = 4
LANES = 128
SLOT_LANE = 120

EPSILON = 1e-05
BF = jnp.bfloat16
F32 = jnp.float32


def layer_norm(values, gain_vec):
    center = values - jnp.sum(values, axis=-1, keepdims=True) * (1.0 / CHAN)
    spread = jnp.sum(center * center, axis=-1, keepdims=True) * (1.0 / CHAN)
    return (center * lax.rsqrt(spread + EPSILON) * gain_vec).astype(BF)


def dot(a, b):
    return jnp.dot(a, b, preferred_element_type=F32)


def dot_t(a, b):
    return lax.dot_general(a, b, (((1,), (1,)), ((), ())), preferred_element_type=F32)


def biases(bias_ref, last_row, queries):
    first = TOK - queries
    base = jnp.concatenate([bias_ref[h][first:] for h in range(HEADS)], axis=0)
    shape = (HEADS * queries, TOK)
    key = lax.broadcasted_iota(jnp.int32, shape, 1)
    query = lax.broadcasted_iota(jnp.int32, shape, 0) % queries + first
    rows_differ = (key // WIN >= SHIFT) != (query // WIN >= SHIFT)
    cols_differ = (key % WIN >= SHIFT) != (query % WIN >= SHIFT)
    row_pen = jnp.where(rows_differ, jnp.where(last_row, -100.0, 0.0).astype(F32), 0.0)
    plain = base + row_pen
    both = base + jnp.where(cols_differ, -100.0, row_pen)
    return plain, both


def head_masks():
    lane = lax.broadcasted_iota(jnp.int32, (1, CHAN), 1)
    return [
        ((lane >= h * HEAD_DIM) & (lane < (h + 1) * HEAD_DIM)).astype(F32) for h in range(HEADS)
    ]


def attend(x, gain, wq, wk, wv, wp, bias_of, queries):
    masks = head_masks()
    low_masks = [m.astype(BF) for m in masks]
    normed = layer_norm(x, gain)
    if queries == TOK:
        x_q, n_q = x, normed
    else:
        pick = lambda a: jnp.concatenate(
            [a[g * TOK + TOK - queries : (g + 1) * TOK] for g in range(GROUP)], axis=0
        )
        x_q, n_q = pick(x), pick(normed)
    q = (dot(n_q, wq) * HEAD_DIM ** (-0.5)).astype(BF)
    k = dot(normed, wk).astype(BF)
    v = dot(normed, wv).astype(BF)
    mixed = []
    for g in range(GROUP):
        q_w = q[g * queries : (g + 1) * queries]
        stacked = jnp.concatenate([q_w * low_masks[h] for h in range(HEADS)], axis=0)
        scores = dot_t(stacked, k[g * TOK : (g + 1) * TOK]) + bias_of(g)
        top = jnp.max(scores, axis=1, keepdims=True)
        grown = jnp.exp(scores - top)
        weights = (grown * (1.0 / jnp.sum(grown, axis=1, keepdims=True))).astype(BF)
        wide = dot(weights, v[g * TOK : (g + 1) * TOK])
        total = wide[:queries] * masks[0]
        for h in range(1, HEADS):
            total = total + wide[h * queries : (h + 1) * queries] * masks[h]
        mixed.append(total)
    mixed = jnp.concatenate(mixed, axis=0).astype(BF)
    return (x_q + dot(mixed, wp)).astype(BF)


def feed(states, gain, wh, wo):
    flat = states.astype(F32)
    normed = layer_norm(flat, gain)
    inner = jax.nn.gelu(dot(normed, wh)).astype(BF)
    return (flat + dot_t(inner, wo)).astype(BF)


def roll_cols(x, by):
    by = by % x.shape[1]
    return jnp.concatenate([x[:, by:], x[:, :by]], axis=1)


def window_at(shifted, i, g, row):
    start = pl.multiple_of((i * GROUP + g) * WIN, WIN)
    return shifted[row : row + WIN, pl.ds(start, WIN), :].reshape(TOK, CHAN)


def group_at(shifted, i):
    return jnp.concatenate([window_at(shifted, i, g, 0) for g in range(GROUP)], axis=0)


def own_kernel(
    pixels, told, bias, gain_a, wq, wk, wv, wp,
    upper, first, rest, prv, facts,
    shifted, nxt_buf, prv_buf, facts_buf, bias_own, send_sem, recv_sem,
):
    bands = lax.axis_size("band")
    me = lax.axis_index("band")
    right, left = lax.rem(me + 1, bands), lax.rem(me + bands - 1, bands)
    rows, cols, _ = pixels.shape
    windows = cols // WIN
    groups = windows // GROUP
    chunks = groups // 2
    width = cols // chunks

    barrier = pltpu.get_barrier_semaphore()
    for neighbour in (left, right):
        pl.semaphore_signal(
            barrier, inc=1, device_id={"band": neighbour}, device_id_type=pl.DeviceIdType.MESH
        )
    pl.semaphore_wait(barrier, 2)
    copies = []
    for c in range(chunks):
        part = pl.ds(c * width, width)
        copies.append(
            pltpu.make_async_remote_copy(
                src_ref=pixels.at[0:SHIFT, part],
                dst_ref=nxt_buf.at[:, part],
                send_sem=send_sem.at[c],
                recv_sem=recv_sem.at[c],
                device_id={"band": left},
                device_id_type=pl.DeviceIdType.MESH,
            )
        )
    copies.append(
        pltpu.make_async_remote_copy(
            src_ref=pixels.at[rows - SHIFT : rows],
            dst_ref=prv_buf,
            send_sem=send_sem.at[chunks],
            recv_sem=recv_sem.at[chunks],
            device_id={"band": right},
            device_id_type=pl.DeviceIdType.MESH,
        )
    )
    copies.append(
        pltpu.make_async_remote_copy(
            src_ref=told,
            dst_ref=facts_buf,
            send_sem=send_sem.at[chunks + 1],
            recv_sem=recv_sem.at[chunks + 1],
            device_id={"band": right},
            device_id_type=pl.DeviceIdType.MESH,
        )
    )
    for copy in copies[:chunks]:
        copy.start()
    copies[chunks + 1].start()

    shifted[0 : WIN - SHIFT] = roll_cols(pixels[SHIFT:].astype(F32), SHIFT)
    bias_own[0], bias_own[1] = biases(bias, me == bands - 1, TOK)

    def step(i, _):
        def edge(g):
            return bias_own[(i * GROUP + g == windows - 1).astype(jnp.int32)]

        own = attend(group_at(shifted, i), gain_a[...], wq[...], wk[...], wv[...], wp[...], edge, TOK)
        for g in range(GROUP):
            w = i * GROUP + g
            value = own[g * TOK : (g + 1) * TOK]
            upper[w] = value[:HALF]
            first[w] = value[:, :LANES]
            rest[w] = value[:, LANES:]
        return 0

    for c in range(chunks):
        copies[c].wait()
        if c == chunks // 2:
            copies[chunks].start()
        low = c * width
        block = nxt_buf[:, low : low + width].astype(F32)
        if c == 0:
            shifted[WIN - SHIFT :, cols - SHIFT :] = block[:, :SHIFT]
            shifted[WIN - SHIFT :, 0 : width - SHIFT] = block[:, SHIFT:]
        else:
            shifted[WIN - SHIFT :, low - SHIFT : low + width - SHIFT] = block
        begin = 2 * c - 1 if c else 0
        end = 2 * c + 1 if c < chunks - 1 else groups
        lax.fori_loop(begin, end, step, 0)
    copies[chunks + 1].wait()
    facts[...] = facts_buf[...]
    copies[chunks].wait()
    prv[...] = prv_buf[...]


def pack_kernel(keep, count, dests, slots, first, rest, outgoing, order):
    bands = lax.axis_size("band")
    windows = first.shape[0]
    tiles = windows // TILE
    pairs = -(-tiles // bands)

    def scan(w, kept):
        order[kept] = w
        return kept + keep[w]

    live = jnp.minimum(lax.fori_loop(0, windows, scan, jnp.int32(0)), count[0])
    if bands * pairs > tiles:
        outgoing[...] = jnp.full(outgoing.shape, CAP, BF)
    lane = lax.broadcasted_iota(jnp.int32, (TOK, LANES), 1)

    def pack(t, _):
        place = dests[t] * pairs + t // bands
        slot = jnp.where(t * TILE < live, slots[t], CAP).astype(F32)
        halves = []
        for p in range(TILE):
            position = t * TILE + p
            valid = position < live
            source = jnp.where(valid, order[jnp.where(valid, position, 0)], 0)
            value = first[source]
            outgoing[place, p * TOK : (p + 1) * TOK] = jnp.where(valid, value, jnp.zeros_like(value))
            tail = rest[source].astype(F32)
            tail = jnp.concatenate([tail, jnp.zeros((TOK, 2 * LANES - CHAN), F32)], axis=1)
            halves.append(jnp.where(valid, tail, 0.0))
        both = jnp.where(lane < TOK, halves[0], pltpu.roll(halves[1], TOK, 1))
        both = jnp.where(lane >= SLOT_LANE, slot, both)
        outgoing[place, TILE * TOK :] = both.astype(BF)
        return 0

    lax.fori_loop(0, tiles, pack, 0)


def map_kernel(
    keep_own, count, facts, pixels, prv, upper, bias, gain_a, wq, wk, wv, wp, gain_m, wh, wo,
    restored,
    shifted, result, bias_prev, act_own, act_prev,
):
    me = lax.axis_index("band")
    windows = pixels.shape[1] // WIN

    def scan(w, carry):
        own, prev = carry
        act_own[w] = ((keep_own[w] == 1) & (own < count[0])).astype(jnp.int32)
        act_prev[w] = ((facts[0, w] == 1) & (prev < facts[0, windows])).astype(jnp.int32)
        return own + keep_own[w], prev + facts[0, w]

    lax.fori_loop(0, windows, scan, (jnp.int32(0), jnp.int32(0)))
    shifted[0:SHIFT] = roll_cols(prv[...].astype(F32), SHIFT)
    shifted[SHIFT:] = roll_cols(pixels[...].astype(F32), SHIFT)
    bias_prev[0], bias_prev[1] = biases(bias, me == 0, HALF)

    def step(i, _):
        def edge(g):
            return bias_prev[(i * GROUP + g == windows - 1).astype(jnp.int32)]

        prev = attend(group_at(shifted, i), gain_a[...], wq[...], wk[...], wv[...], wp[...], edge, HALF)
        states = jnp.concatenate([upper[i * GROUP + g] for g in range(GROUP)] + [prev], axis=0)
        done = feed(states, gain_m[...], wh[...], wo[...]).astype(F32)
        for g in range(GROUP):
            w = i * GROUP + g
            cols = pl.ds(pl.multiple_of(w * WIN, WIN), WIN)
            upper_new = done[g * HALF : (g + 1) * HALF].reshape(SHIFT, WIN, CHAN)
            lower_new = done[(GROUP + g) * HALF : (GROUP + g + 1) * HALF].reshape(SHIFT, WIN, CHAN)
            result[0:SHIFT, cols, :] = jnp.where(
                act_prev[w] == 1, lower_new, shifted[SHIFT : 2 * SHIFT, cols, :]
            )
            result[SHIFT:, cols, :] = jnp.where(
                act_own[w] == 1, upper_new, shifted[2 * SHIFT :, cols, :]
            )
        return 0

    lax.fori_loop(0, windows // GROUP, step, 0)
    restored[...] = roll_cols(result[...], -SHIFT).astype(BF)


def place_kernel(incoming, work):
    work[...] = jnp.zeros(work.shape, BF)
    lane = lax.broadcasted_iota(jnp.int32, (16, LANES), 1)

    def put(t, _):
        head = incoming[t, TILE * TOK : TILE * TOK + 16].astype(F32)
        slot = jnp.max(jnp.where(lane >= SLOT_LANE, head, 0.0)).astype(jnp.int32)

        @pl.when(slot < CAP)
        def _():
            tail = incoming[t, TILE * TOK :].astype(F32)
            work[slot, :, :LANES] = incoming[t, : TILE * TOK]
            work[slot, :TOK, LANES:] = tail[:, : CHAN - LANES].astype(BF)
            work[slot, TOK:, LANES:] = pltpu.roll(tail, TOK, 1)[:, : CHAN - LANES].astype(BF)

        return 0

    lax.fori_loop(0, incoming.shape[0], put, 0)


def position_bias(bias_table):
    coords = jnp.arange(TOK, dtype=jnp.int32)
    row_pos, col_pos = coords // WIN, coords % WIN
    index = (row_pos[:, None] - row_pos[None, :] + WIN - 1) * (2 * WIN - 1) + (
        col_pos[:, None] - col_pos[None, :] + WIN - 1
    )
    entries = bias_table.shape[0]
    onehot = (jnp.arange(entries, dtype=jnp.int32)[:, None] == index.reshape(1, -1)).astype(F32)
    return jnp.dot(bias_table.T, onehot, precision=lax.Precision.HIGHEST).reshape(HEADS, TOK, TOK)


def shards(
    pixels, keep_mask, band_counts, plan_dest, plan_slot, bias_table, gain_attn, qkv_weight,
    proj_weight, gain_mlp, hidden_weight, output_weight,
):
    bands = lax.axis_size("band")
    rows, cols, channels = pixels.shape
    windows = cols // WIN
    tiles = windows // TILE
    pairs = -(-tiles // bands)
    told = jnp.concatenate([keep_mask[0], band_counts])
    told = jnp.pad(told, (0, -told.shape[0] % LANES))[None]
    bias = position_bias(bias_table)
    wq, wk, wv = (qkv_weight[:, i * CHAN : (i + 1) * CHAN] for i in range(3))
    smem = pl.BlockSpec(memory_space=pltpu.SMEM)
    vmem = pl.BlockSpec(memory_space=pltpu.VMEM)
    limit = pltpu.CompilerParams(vmem_limit_bytes=63 * 1024 * 1024)
    chunks = windows // GROUP // 2
    upper, first, rest, prv, facts = pl.pallas_call(
        own_kernel,
        out_shape=(
            jax.ShapeDtypeStruct((windows, HALF, channels), BF),
            jax.ShapeDtypeStruct((windows, TOK, LANES), BF),
            jax.ShapeDtypeStruct((windows, TOK, channels - LANES), BF),
            jax.ShapeDtypeStruct((SHIFT, cols, channels), BF),
            jax.ShapeDtypeStruct(told.shape, jnp.int32),
        ),
        in_specs=[vmem] * 8,
        out_specs=(vmem,) * 5,
        scratch_shapes=[
            pltpu.VMEM((rows, cols, channels), F32),
            pltpu.VMEM((SHIFT, cols, channels), BF),
            pltpu.VMEM((SHIFT, cols, channels), BF),
            pltpu.VMEM(told.shape, jnp.int32),
            pltpu.VMEM((2, HEADS * TOK, TOK), F32),
            pltpu.SemaphoreType.DMA((chunks + 2,)),
            pltpu.SemaphoreType.DMA((chunks + 2,)),
        ],
        compiler_params=pltpu.CompilerParams(
            vmem_limit_bytes=63 * 1024 * 1024, collective_id=0, has_side_effects=True
        ),
        cost_estimate=pl.CostEstimate(flops=3 * 10**9, bytes_accessed=10**7, transcendentals=10**6),
        name="own",
    )(pixels, told, bias, gain_attn[None], wq, wk, wv, proj_weight)
    outgoing = pl.pallas_call(
        pack_kernel,
        out_shape=jax.ShapeDtypeStruct((bands * pairs, TILE * TOK + TOK, LANES), BF),
        in_specs=[smem] * 4 + [vmem] * 2,
        out_specs=vmem,
        scratch_shapes=[pltpu.SMEM((windows + 1,), jnp.int32)],
        compiler_params=limit,
        name="pack",
    )(keep_mask[0], band_counts, plan_dest[0], plan_slot[0], first, rest)
    incoming = lax.all_to_all(
        outgoing.reshape(bands, -1, LANES), "band", split_axis=0, concat_axis=0, tiled=True
    ).reshape(outgoing.shape)
    restored = pl.pallas_call(
        map_kernel,
        out_shape=jax.ShapeDtypeStruct((rows, cols, channels), BF),
        in_specs=[smem] * 3 + [vmem] * 12,
        out_specs=vmem,
        scratch_shapes=[
            pltpu.VMEM((rows + SHIFT, cols, channels), F32),
            pltpu.VMEM((rows, cols, channels), F32),
            pltpu.VMEM((2, HEADS * HALF, TOK), F32),
            pltpu.SMEM((windows,), jnp.int32),
            pltpu.SMEM((windows,), jnp.int32),
        ],
        compiler_params=limit,
        cost_estimate=pl.CostEstimate(flops=10**10, bytes_accessed=3 * 10**7, transcendentals=10**6),
        name="map",
    )(
        keep_mask[0], band_counts, facts, pixels, prv, upper, bias, gain_attn[None], wq, wk, wv,
        proj_weight, gain_mlp[None], hidden_weight, output_weight.T,
    )
    work = pl.pallas_call(
        place_kernel,
        out_shape=jax.ShapeDtypeStruct((CAP, TILE * TOK, channels), BF),
        in_specs=[vmem],
        out_specs=vmem,
        compiler_params=pltpu.CompilerParams(vmem_limit_bytes=16 * 1024 * 1024),
        name="place",
    )(incoming)
    return restored, work


def solution(mesh):
    split = P(("img", "band"))
    in_specs = (split,) * 5 + (P(),) * 7
    return jax.shard_map(shards, mesh=mesh, in_specs=in_specs, out_specs=(split, split), check_vma=False)
```

```python
import jax
import jax.numpy as jnp
from jax import lax
from jax.experimental import pallas as pl
from jax.experimental.pallas import tpu as pltpu
from jax.sharding import PartitionSpec as P

CHAN = 180
HEADS = 6
WIN = 8
TILE = 2
SHIFT = 4
CAP = 8
TOK = WIN * WIN
HALF = TOK // 2
HEAD_DIM = CHAN // HEADS
GROUP = 4
LANES = 128
SLOT_LANE = 120

EPSILON = 1e-05
BF = jnp.bfloat16
F32 = jnp.float32


def layer_norm(values, gain_vec):
    center = values - jnp.sum(values, axis=-1, keepdims=True) * (1.0 / CHAN)
    spread = jnp.sum(center * center, axis=-1, keepdims=True) * (1.0 / CHAN)
    return (center * lax.rsqrt(spread + EPSILON) * gain_vec).astype(BF)


def dot(a, b):
    return jnp.dot(a, b, preferred_element_type=F32)


def dot_t(a, b):
    return lax.dot_general(a, b, (((1,), (1,)), ((), ())), preferred_element_type=F32)


def biases(bias_ref, last_row, queries):
    first = TOK - queries
    base = jnp.concatenate([bias_ref[h][first:] for h in range(HEADS)], axis=0)
    shape = (HEADS * queries, TOK)
    key = lax.broadcasted_iota(jnp.int32, shape, 1)
    query = lax.broadcasted_iota(jnp.int32, shape, 0) % queries + first
    rows_differ = (key // WIN >= SHIFT) != (query // WIN >= SHIFT)
    cols_differ = (key % WIN >= SHIFT) != (query % WIN >= SHIFT)
    row_pen = jnp.where(rows_differ, jnp.where(last_row, -100.0, 0.0).astype(F32), 0.0)
    plain = base + row_pen
    both = base + jnp.where(cols_differ, -100.0, row_pen)
    return plain, both


def head_masks():
    lane = lax.broadcasted_iota(jnp.int32, (1, CHAN), 1)
    return [
        ((lane >= h * HEAD_DIM) & (lane < (h + 1) * HEAD_DIM)).astype(F32) for h in range(HEADS)
    ]


def attend(x, gain, wq, wk, wv, wp, bias_of, queries):
    masks = head_masks()
    low_masks = [m.astype(BF) for m in masks]
    normed = layer_norm(x, gain)
    if queries == TOK:
        x_q, n_q = x, normed
    else:
        pick = lambda a: jnp.concatenate(
            [a[g * TOK + TOK - queries : (g + 1) * TOK] for g in range(GROUP)], axis=0
        )
        x_q, n_q = pick(x), pick(normed)
    q = (dot(n_q, wq) * HEAD_DIM ** (-0.5)).astype(BF)
    k = dot(normed, wk).astype(BF)
    v = dot(normed, wv).astype(BF)
    mixed = []
    for g in range(GROUP):
        q_w = q[g * queries : (g + 1) * queries]
        stacked = jnp.concatenate([q_w * low_masks[h] for h in range(HEADS)], axis=0)
        scores = dot_t(stacked, k[g * TOK : (g + 1) * TOK]) + bias_of(g)
        top = jnp.max(scores, axis=1, keepdims=True)
        grown = jnp.exp(scores - top)
        weights = (grown * (1.0 / jnp.sum(grown, axis=1, keepdims=True))).astype(BF)
        wide = dot(weights, v[g * TOK : (g + 1) * TOK])
        total = wide[:queries] * masks[0]
        for h in range(1, HEADS):
            total = total + wide[h * queries : (h + 1) * queries] * masks[h]
        mixed.append(total)
    mixed = jnp.concatenate(mixed, axis=0).astype(BF)
    return (x_q + dot(mixed, wp)).astype(BF)


def feed(states, gain, wh, wo):
    flat = states.astype(F32)
    normed = layer_norm(flat, gain)
    inner = jax.nn.gelu(dot(normed, wh)).astype(BF)
    return (flat + dot_t(inner, wo)).astype(BF)


def roll_cols(x, by):
    by = by % x.shape[1]
    return jnp.concatenate([x[:, by:], x[:, :by]], axis=1)


def window_at(shifted, i, g, row):
    start = pl.multiple_of((i * GROUP + g) * WIN, WIN)
    return shifted[row : row + WIN, pl.ds(start, WIN), :].reshape(TOK, CHAN)


def group_at(shifted, i):
    return jnp.concatenate([window_at(shifted, i, g, 0) for g in range(GROUP)], axis=0)


def own_kernel(
    pixels, told, bias, gain_a, wq, wk, wv, wp,
    upper, first, rest, prv, facts,
    shifted, nxt_buf, prv_buf, facts_buf, bias_own, send_sem, recv_sem,
):
    bands = lax.axis_size("band")
    me = lax.axis_index("band")
    right, left = lax.rem(me + 1, bands), lax.rem(me + bands - 1, bands)
    rows, cols, _ = pixels.shape
    windows = cols // WIN
    groups = windows // GROUP
    chunks = groups // 2
    width = cols // chunks

    barrier = pltpu.get_barrier_semaphore()
    for neighbour in (left, right):
        pl.semaphore_signal(
            barrier, inc=1, device_id={"band": neighbour}, device_id_type=pl.DeviceIdType.MESH
        )
    pl.semaphore_wait(barrier, 2)
    copies = []
    for c in range(chunks):
        part = pl.ds(c * width, width)
        copies.append(
            pltpu.make_async_remote_copy(
                src_ref=pixels.at[0:SHIFT, part],
                dst_ref=nxt_buf.at[:, part],
                send_sem=send_sem.at[c],
                recv_sem=recv_sem.at[c],
                device_id={"band": left},
                device_id_type=pl.DeviceIdType.MESH,
            )
        )
    copies.append(
        pltpu.make_async_remote_copy(
            src_ref=pixels.at[rows - SHIFT : rows],
            dst_ref=prv_buf,
            send_sem=send_sem.at[chunks],
            recv_sem=recv_sem.at[chunks],
            device_id={"band": right},
            device_id_type=pl.DeviceIdType.MESH,
        )
    )
    copies.append(
        pltpu.make_async_remote_copy(
            src_ref=told,
            dst_ref=facts_buf,
            send_sem=send_sem.at[chunks + 1],
            recv_sem=recv_sem.at[chunks + 1],
            device_id={"band": right},
            device_id_type=pl.DeviceIdType.MESH,
        )
    )
    for copy in copies[:chunks]:
        copy.start()
    copies[chunks + 1].start()

    shifted[0 : WIN - SHIFT] = roll_cols(pixels[SHIFT:].astype(F32), SHIFT)
    bias_own[0], bias_own[1] = biases(bias, me == bands - 1, TOK)

    def step(i, _):
        def edge(g):
            return bias_own[(i * GROUP + g == windows - 1).astype(jnp.int32)]

        own = attend(group_at(shifted, i), gain_a[...], wq[...], wk[...], wv[...], wp[...], edge, TOK)
        for g in range(GROUP):
            w = i * GROUP + g
            value = own[g * TOK : (g + 1) * TOK]
            upper[w] = value[:HALF]
            first[w] = value[:, :LANES]
            rest[w] = value[:, LANES:]
        return 0

    for c in range(chunks):
        copies[c].wait()
        if c == chunks // 4:
            copies[chunks].start()
        low = c * width
        block = nxt_buf[:, low : low + width].astype(F32)
        if c == 0:
            shifted[WIN - SHIFT :, cols - SHIFT :] = block[:, :SHIFT]
            shifted[WIN - SHIFT :, 0 : width - SHIFT] = block[:, SHIFT:]
        else:
            shifted[WIN - SHIFT :, low - SHIFT : low + width - SHIFT] = block
        begin = 2 * c - 1 if c else 0
        end = 2 * c + 1 if c < chunks - 1 else groups
        lax.fori_loop(begin, end, step, 0)
    copies[chunks + 1].wait()
    facts[...] = facts_buf[...]
    copies[chunks].wait()
    prv[...] = prv_buf[...]


def pack_kernel(keep, count, dests, slots, first, rest, outgoing, order):
    bands = lax.axis_size("band")
    windows = first.shape[0]
    tiles = windows // TILE
    pairs = -(-tiles // bands)

    def scan(w, kept):
        order[kept] = w
        return kept + keep[w]

    live = jnp.minimum(lax.fori_loop(0, windows, scan, jnp.int32(0)), count[0])
    if bands * pairs > tiles:
        outgoing[...] = jnp.full(outgoing.shape, CAP, BF)
    lane = lax.broadcasted_iota(jnp.int32, (TOK, LANES), 1)

    def pack(t, _):
        place = dests[t] * pairs + t // bands
        slot = jnp.where(t * TILE < live, slots[t], CAP).astype(F32)
        halves = []
        for p in range(TILE):
            position = t * TILE + p
            valid = position < live
            source = jnp.where(valid, order[jnp.where(valid, position, 0)], 0)
            value = first[source]
            outgoing[place, p * TOK : (p + 1) * TOK] = jnp.where(valid, value, jnp.zeros_like(value))
            tail = rest[source].astype(F32)
            tail = jnp.concatenate([tail, jnp.zeros((TOK, 2 * LANES - CHAN), F32)], axis=1)
            halves.append(jnp.where(valid, tail, 0.0))
        both = jnp.where(lane < TOK, halves[0], pltpu.roll(halves[1], TOK, 1))
        both = jnp.where(lane >= SLOT_LANE, slot, both)
        outgoing[place, TILE * TOK :] = both.astype(BF)
        return 0

    lax.fori_loop(0, tiles, pack, 0)


def map_kernel(
    keep_own, count, facts, pixels, prv, upper, bias, gain_a, wq, wk, wv, wp, gain_m, wh, wo,
    restored,
    shifted, result, bias_prev, act_own, act_prev,
):
    me = lax.axis_index("band")
    windows = pixels.shape[1] // WIN

    def scan(w, carry):
        own, prev = carry
        act_own[w] = ((keep_own[w] == 1) & (own < count[0])).astype(jnp.int32)
        act_prev[w] = ((facts[0, w] == 1) & (prev < facts[0, windows])).astype(jnp.int32)
        return own + keep_own[w], prev + facts[0, w]

    lax.fori_loop(0, windows, scan, (jnp.int32(0), jnp.int32(0)))
    shifted[0:SHIFT] = roll_cols(prv[...].astype(F32), SHIFT)
    shifted[SHIFT:] = roll_cols(pixels[...].astype(F32), SHIFT)
    bias_prev[0], bias_prev[1] = biases(bias, me == 0, HALF)

    def step(i, _):
        def edge(g):
            return bias_prev[(i * GROUP + g == windows - 1).astype(jnp.int32)]

        prev = attend(group_at(shifted, i), gain_a[...], wq[...], wk[...], wv[...], wp[...], edge, HALF)
        states = jnp.concatenate([upper[i * GROUP + g] for g in range(GROUP)] + [prev], axis=0)
        done = feed(states, gain_m[...], wh[...], wo[...]).astype(F32)
        for g in range(GROUP):
            w = i * GROUP + g
            cols = pl.ds(pl.multiple_of(w * WIN, WIN), WIN)
            upper_new = done[g * HALF : (g + 1) * HALF].reshape(SHIFT, WIN, CHAN)
            lower_new = done[(GROUP + g) * HALF : (GROUP + g + 1) * HALF].reshape(SHIFT, WIN, CHAN)
            result[0:SHIFT, cols, :] = jnp.where(
                act_prev[w] == 1, lower_new, shifted[SHIFT : 2 * SHIFT, cols, :]
            )
            result[SHIFT:, cols, :] = jnp.where(
                act_own[w] == 1, upper_new, shifted[2 * SHIFT :, cols, :]
            )
        return 0

    lax.fori_loop(0, windows // GROUP, step, 0)
    restored[...] = roll_cols(result[...], -SHIFT).astype(BF)


def place_kernel(incoming, work):
    work[...] = jnp.zeros(work.shape, BF)
    lane = lax.broadcasted_iota(jnp.int32, (16, LANES), 1)

    def put(t, _):
        head = incoming[t, TILE * TOK : TILE * TOK + 16].astype(F32)
        slot = jnp.max(jnp.where(lane >= SLOT_LANE, head, 0.0)).astype(jnp.int32)

        @pl.when(slot < CAP)
        def _():
            tail = incoming[t, TILE * TOK :].astype(F32)
            work[slot, :, :LANES] = incoming[t, : TILE * TOK]
            work[slot, :TOK, LANES:] = tail[:, : CHAN - LANES].astype(BF)
            work[slot, TOK:, LANES:] = pltpu.roll(tail, TOK, 1)[:, : CHAN - LANES].astype(BF)

        return 0

    lax.fori_loop(0, incoming.shape[0], put, 0)


def position_bias(bias_table):
    coords = jnp.arange(TOK, dtype=jnp.int32)
    row_pos, col_pos = coords // WIN, coords % WIN
    index = (row_pos[:, None] - row_pos[None, :] + WIN - 1) * (2 * WIN - 1) + (
        col_pos[:, None] - col_pos[None, :] + WIN - 1
    )
    entries = bias_table.shape[0]
    onehot = (jnp.arange(entries, dtype=jnp.int32)[:, None] == index.reshape(1, -1)).astype(F32)
    return jnp.dot(bias_table.T, onehot, precision=lax.Precision.HIGHEST).reshape(HEADS, TOK, TOK)


def shards(
    pixels, keep_mask, band_counts, plan_dest, plan_slot, bias_table, gain_attn, qkv_weight,
    proj_weight, gain_mlp, hidden_weight, output_weight,
):
    bands = lax.axis_size("band")
    rows, cols, channels = pixels.shape
    windows = cols // WIN
    tiles = windows // TILE
    pairs = -(-tiles // bands)
    told = jnp.concatenate([keep_mask[0], band_counts])
    told = jnp.pad(told, (0, -told.shape[0] % LANES))[None]
    bias = position_bias(bias_table)
    wq, wk, wv = (qkv_weight[:, i * CHAN : (i + 1) * CHAN] for i in range(3))
    smem = pl.BlockSpec(memory_space=pltpu.SMEM)
    vmem = pl.BlockSpec(memory_space=pltpu.VMEM)
    limit = pltpu.CompilerParams(vmem_limit_bytes=63 * 1024 * 1024)
    chunks = windows // GROUP // 2
    upper, first, rest, prv, facts = pl.pallas_call(
        own_kernel,
        out_shape=(
            jax.ShapeDtypeStruct((windows, HALF, channels), BF),
            jax.ShapeDtypeStruct((windows, TOK, LANES), BF),
            jax.ShapeDtypeStruct((windows, TOK, channels - LANES), BF),
            jax.ShapeDtypeStruct((SHIFT, cols, channels), BF),
            jax.ShapeDtypeStruct(told.shape, jnp.int32),
        ),
        in_specs=[vmem] * 8,
        out_specs=(vmem,) * 5,
        scratch_shapes=[
            pltpu.VMEM((rows, cols, channels), F32),
            pltpu.VMEM((SHIFT, cols, channels), BF),
            pltpu.VMEM((SHIFT, cols, channels), BF),
            pltpu.VMEM(told.shape, jnp.int32),
            pltpu.VMEM((2, HEADS * TOK, TOK), F32),
            pltpu.SemaphoreType.DMA((chunks + 2,)),
            pltpu.SemaphoreType.DMA((chunks + 2,)),
        ],
        compiler_params=pltpu.CompilerParams(
            vmem_limit_bytes=63 * 1024 * 1024, collective_id=0, has_side_effects=True
        ),
        cost_estimate=pl.CostEstimate(flops=3 * 10**9, bytes_accessed=10**7, transcendentals=10**6),
        name="own",
    )(pixels, told, bias, gain_attn[None], wq, wk, wv, proj_weight)
    outgoing = pl.pallas_call(
        pack_kernel,
        out_shape=jax.ShapeDtypeStruct((bands * pairs, TILE * TOK + TOK, LANES), BF),
        in_specs=[smem] * 4 + [vmem] * 2,
        out_specs=vmem,
        scratch_shapes=[pltpu.SMEM((windows + 1,), jnp.int32)],
        compiler_params=limit,
        name="pack",
    )(keep_mask[0], band_counts, plan_dest[0], plan_slot[0], first, rest)
    incoming = lax.all_to_all(
        outgoing.reshape(bands, -1, LANES), "band", split_axis=0, concat_axis=0, tiled=True
    ).reshape(outgoing.shape)
    restored = pl.pallas_call(
        map_kernel,
        out_shape=jax.ShapeDtypeStruct((rows, cols, channels), BF),
        in_specs=[smem] * 3 + [vmem] * 12,
        out_specs=vmem,
        scratch_shapes=[
            pltpu.VMEM((rows + SHIFT, cols, channels), F32),
            pltpu.VMEM((rows, cols, channels), F32),
            pltpu.VMEM((2, HEADS * HALF, TOK), F32),
            pltpu.SMEM((windows,), jnp.int32),
            pltpu.SMEM((windows,), jnp.int32),
        ],
        compiler_params=limit,
        cost_estimate=pl.CostEstimate(flops=10**10, bytes_accessed=3 * 10**7, transcendentals=10**6),
        name="map",
    )(
        keep_mask[0], band_counts, facts, pixels, prv, upper, bias, gain_attn[None], wq, wk, wv,
        proj_weight, gain_mlp[None], hidden_weight, output_weight.T,
    )
    work = pl.pallas_call(
        place_kernel,
        out_shape=jax.ShapeDtypeStruct((CAP, TILE * TOK, channels), BF),
        in_specs=[vmem],
        out_specs=vmem,
        compiler_params=pltpu.CompilerParams(vmem_limit_bytes=16 * 1024 * 1024),
        name="place",
    )(incoming)
    return restored, work


def solution(mesh):
    split = P(("img", "band"))
    in_specs = (split,) * 5 + (P(),) * 7
    return jax.shard_map(shards, mesh=mesh, in_specs=in_specs, out_specs=(split, split), check_vma=False)
```
